32 devices in a mesh: ex: 32 (over z, y, x, core), cls: 1.
Axes of the slice: x: 2, y: 2, z: 4, core: 2. Of those that a mesh axis runs over, the one named last changes fastest.
Arguments:
- features: bfloat16 [32768, 1664], P('ex'), may hold values from -16 to 16
- labels: int32 [32768], P('ex'), may hold values from 0 to 1407
- weight: bfloat16 [1664, 1408], P(None, 'cls'), may hold values from -1 to 1
- noise: bfloat16 [1664, 1408], P('ex', 'cls'), may hold values from -5 to 5
Outputs:
- new_weight: bfloat16 [1664, 1408], P(None, 'cls')
The draws below stay inside these ranges and needn't reach their ends.
All inputs are finite; a program needn't handle non-finite values.
Results may differ from the reference program's by a relative error of at most 0.0013.
Values may be sent and summed in bfloat16 or wider, within the bound.
No kernel may reach another device: no remote copies, remote signals or barrier semaphores. Data moves between devices by JAX's collectives and lax.ppermute only.
A program may use at most 128 MiB of HBM per device.

```python
import jax
import jax.numpy as jnp
from jax import lax

D = 1664
B_DEV = 1024
CLASSES = 1408
BATCH = 32768
N_EX = 32


def shared_weight(key):
    base = jax.random.normal(jax.random.fold_in(key, 11), (D, CLASSES), jnp.float32)
    return jnp.clip(base * (9.0 / D) ** 0.5, -1.0, 1.0)


def draw_weight(key, part):
    return shared_weight(key).astype(jnp.bfloat16)


def draw_features(key, part):
    table = shared_weight(key).astype(jnp.bfloat16).astype(jnp.float32)
    drawn = jnp.clip(jax.random.normal(jax.random.fold_in(key, 12), (BATCH, D), jnp.float32), -6.0, 6.0)
    first = jax.random.randint(jax.random.fold_in(key, 14), (BATCH,), 0, CLASSES)
    second = (first + 1 + jax.random.randint(jax.random.fold_in(key, 15), (BATCH,), 0, CLASSES - 1)) % CLASSES
    row_ids = jnp.arange(BATCH, dtype=jnp.int32)
    strength = 110.0 + 105.0 * (row_ids // 64 % 3).astype(jnp.float32)
    picked = (row_ids % 64 == 5) | (row_ids % 64 == 37)
    col_a = jnp.take(table, first, axis=1).T
    col_b = jnp.take(table, second, axis=1).T
    aligned = (strength[:, None] * col_a + (strength[:, None] - 2.0) * col_b) / 9.0 + 0.05 * drawn
    result = jnp.where(picked[:, None], aligned, drawn)
    return jnp.clip(result, -16.0, 16.0).astype(jnp.bfloat16)


def plant(drawn, stream_key, least, largest):
    shape = drawn.shape
    spot = [jax.random.randint(jax.random.fold_in(stream_key, axis), (), 0, shape[axis]) for axis in range(len(shape))]
    drawn = drawn.at[tuple(spot)].set(least)
    longest = shape.index(max(shape))
    spot[longest] = (spot[longest] + 1) % shape[longest]
    return drawn.at[tuple(spot)].set(largest)


def level_of(rng, shape, cuts, smallest, high):
    def one(position, parts):
        steps = jax.random.uniform(jax.random.fold_in(jax.random.fold_in(rng, 6), position), (parts,), jnp.float32, smallest / len(cuts), high / len(cuts))
        return jnp.repeat(jnp.exp(steps), shape[position] // parts).reshape((-1,) + (1,) * (len(shape) - position - 1))

    gain = one(*cuts[0])
    for cut in cuts[1:]:
        gain = gain * one(*cut)
    return gain


def gaussian(stream_key, shape, deviation, bound, cuts=(), kind=jnp.bfloat16):
    values = deviation * jax.random.normal(stream_key, shape, jnp.float32)
    if cuts:
        values = values * level_of(stream_key, shape, cuts, -0.22, 0.18)
    return jnp.clip(values, -bound, bound).astype(kind)


def setup_inputs(seed: int = 0) -> dict:
    arg_keys = jax.random.split(jax.random.key(seed), 5)
    return {
        "features": draw_features(jax.random.fold_in(arg_keys[4], 71), 0),
        "labels": plant(jax.random.randint(arg_keys[1], (BATCH,), 0, CLASSES), jax.random.fold_in(arg_keys[1], 1), 0, CLASSES - 1).astype(jnp.int32),
        "weight": draw_weight(jax.random.fold_in(arg_keys[4], 71), 0),
        "noise": gaussian(arg_keys[3], (D, CLASSES), 1.0, 5.0, ((0, 32),)),
    }


def reference(features, labels, weight, noise):
    clip_norm = 48.0
    blocks_x = features.reshape(N_EX, B_DEV, D)
    blocks_l = labels.reshape(N_EX, B_DEV)
    classes_row = jnp.arange(CLASSES, dtype=jnp.int32)

    def accumulate(total, item):
        rows, labs = item
        logits = jnp.dot(rows, weight, preferred_element_type=jnp.float32)
        probs = jax.nn.softmax(logits, axis=1)
        onehot = (classes_row[None, :] == labs[:, None]).astype(jnp.float32)
        resid = probs - onehot
        resid_norm = jnp.sqrt(lax.optimization_barrier(jnp.sum(resid * resid, axis=1)))
        feat = rows.astype(jnp.float32)
        feat_norm = jnp.sqrt(lax.optimization_barrier(jnp.sum(feat * feat, axis=1)))
        factor = clip_norm / jnp.maximum(feat_norm * resid_norm, clip_norm)
        coef = (factor[:, None] * resid).astype(jnp.bfloat16)
        part = lax.dot_general(rows, coef, (((0,), (0,)), ((), ())), preferred_element_type=jnp.float32)
        return (total + part, None)
    grad, _ = lax.scan(accumulate, jnp.zeros((D, CLASSES), jnp.float32), (blocks_x, blocks_l))
    scale = 0.1 * CLASSES / BATCH
    updated = weight.astype(jnp.float32) - scale * (grad + 0.96 * clip_norm * noise.astype(jnp.float32))
    return updated.astype(jnp.bfloat16)
```

```python
import functools

import jax
import jax.numpy as jnp
from jax import lax
from jax.experimental import pallas as pl
from jax.experimental.pallas import tpu as pltpu
from jax.sharding import PartitionSpec as P

CLIP = 48.0
SIDES = 4
ROW = 8


def coefficients(features, labels, weight):
    cls_width = weight.shape[1]
    logits = jnp.dot(features, weight, preferred_element_type=jnp.float32)
    offset = lax.axis_index("cls") * cls_width
    local_lab = labels - offset
    columns = lax.broadcasted_iota(jnp.int32, (1, cls_width), 1)
    onehot = columns == local_lab[:, None]
    label_part = jnp.sum(jnp.where(onehot, logits, 0.0), axis=1)
    top = lax.pmax(jnp.max(logits, axis=1), "cls")
    expo = jnp.exp(logits - top[:, None])
    total, squares, label_logit = lax.psum(
        (jnp.sum(expo, axis=1), jnp.sum(expo * expo, axis=1), label_part), "cls"
    )
    probs = expo / total[:, None]
    label_prob = jnp.exp(label_logit - top) / total
    resid_sq = squares / (total * total) - 2.0 * label_prob + 1.0
    resid_norm = jnp.sqrt(jnp.maximum(resid_sq, 0.0))
    feat = features.astype(jnp.float32)
    feat_norm = jnp.sqrt(jnp.sum(feat * feat, axis=1))
    factor = CLIP / jnp.maximum(feat_norm * resid_norm, CLIP)
    resid = probs - onehot.astype(jnp.float32)
    return (factor[:, None] * resid).astype(jnp.bfloat16)


def place_kernel(rows, offsets_ref, *refs):
    blocks, out_ref, sems = refs[:-2], refs[-2], refs[-1]
    copies = []
    for i, block in enumerate(blocks):
        start = pl.multiple_of(offsets_ref[i] * rows, ROW)
        copies.append(
            pltpu.make_async_copy(block, out_ref.at[pl.ds(start, rows), :], sems.at[i])
        )
    for copy in copies:
        copy.start()
    for copy in copies:
        copy.wait()


def place(blocks, offsets, total):
    rows, width = blocks[0].shape
    grid_spec = pltpu.PrefetchScalarGridSpec(
        num_scalar_prefetch=1,
        grid=(1,),
        in_specs=[
            pl.BlockSpec((rows, width), lambda i, off: (0, 0)) for _ in blocks
        ],
        out_specs=pl.BlockSpec(memory_space=pl.ANY),
        scratch_shapes=[pltpu.SemaphoreType.DMA((len(blocks),))],
    )
    return pl.pallas_call(
        functools.partial(place_kernel, rows),
        grid_spec=grid_spec,
        out_shape=jax.ShapeDtypeStruct((total, width), blocks[0].dtype),
    )(offsets, *blocks)


def by_rows(features, labels, weight, noise):
    bf16, f32 = jnp.bfloat16, jnp.float32
    n = lax.axis_size("ex")
    depth, width = weight.shape
    coef = coefficients(features, labels, weight)
    partial_grad = lax.dot_general(
        features, coef, (((0,), (0,)), ((), ())), preferred_element_type=f32
    )
    me = lax.axis_index("ex")
    layers = n // (2 * SIDES)
    half, side, own = depth // 2, depth // (2 * SIDES), depth // n
    core, pos_a, pos_b, layer = me % 2, me // 2 % 2, me // 4 % 2, me // 8

    def swap(x, pairs):
        return lax.ppermute(x, "ex", pairs)

    cores = [(i, i ^ 1) for i in range(n)]
    first = [(i, i ^ (4 if i % 2 else 2)) for i in range(n)]
    second = [(i, i ^ (2 if i % 2 else 4)) for i in range(n)]
    layer_swaps = [[(i, i ^ (8 * d)) for i in range(n)] for d in range(1, layers)]

    target = []
    for d in range(n):
        c, q, k = d // (SIDES * layers), d // layers % SIDES, d % layers
        target.append((d, k * 2 * SIDES + q * 2 + c))
    noise_own = swap(noise, target)

    def block_index(far_first, far_second):
        flip_a = jnp.where(core == 0, far_first, far_second)
        flip_b = jnp.where(core == 0, far_second, far_first)
        return (pos_a ^ flip_a) + 2 * (pos_b ^ flip_b)

    def rows_of(x, start, count):
        return lax.dynamic_slice_in_dim(x, start, count, 0)

    sent = rows_of(partial_grad, half * (1 - core), half).astype(bf16)
    got = swap(sent, cores)
    kept = rows_of(partial_grad, half * core, half) + got.astype(f32)

    def side_of(far_first, far_second):
        return rows_of(kept, side * block_index(far_first, far_second), side)

    got_far = swap(side_of(1, 1).astype(bf16), first)
    got_near = swap(side_of(1, 0).astype(bf16), first)
    got_second = swap((side_of(0, 1) + got_far.astype(f32)).astype(bf16), second)
    summed = side_of(0, 0) + got_near.astype(f32) + got_second.astype(f32)

    starts = [own * k // ROW * ROW for k in range(layers)]
    window = max(
        -(-own * (k + 1) // ROW) * ROW - starts[k] for k in range(layers)
    )
    starts = [min(s, side - window) for s in starts]
    table = jnp.asarray(starts, jnp.int32)

    def window_of(k):
        return rows_of(summed, table[k], window)

    grad = window_of(layer)
    for d in range(1, layers):
        grad = grad + swap(window_of(layer ^ d).astype(bf16), layer_swaps[d - 1]).astype(f32)

    inner = own * layer - table[layer]
    noise_rows = lax.dynamic_update_slice_in_dim(
        jnp.zeros((window, width), noise.dtype), noise_own, inner, 0
    )
    begin = half * core + side * block_index(0, 0) + table[layer]
    own_weight = rows_of(weight, begin, window)
    classes = width * lax.axis_size("cls")
    batch = features.shape[0] * n
    scale = 0.1 * classes / batch
    updated = own_weight.astype(f32) - scale * (
        grad + 0.96 * CLIP * noise_rows.astype(f32)
    )
    updated = updated.astype(bf16)

    parts = [updated] + [swap(updated, layer_swaps[d - 1]) for d in range(1, layers)]
    ordered = []
    for k in range(layers):
        piece = lax.select_n(jnp.broadcast_to(layer ^ k, parts[0].shape), *parts)
        skip = own * k - starts[k]
        ordered.append(piece[skip : skip + own])
    mine = jnp.concatenate(ordered, axis=0)
    from_second = swap(mine, second)
    from_first = swap(mine, first)
    from_both = swap(from_second, first)
    here = [mine, from_second, from_first, from_both]
    there = [swap(block, cores) for block in here]
    flips = [(0, 0), (0, 1), (1, 0), (1, 1)]
    offsets = [SIDES * core + block_index(*f) for f in flips]
    offsets += [SIDES * (1 - core) + block_index(f[1], f[0]) for f in flips]
    return place(here + there, jnp.stack(offsets).astype(jnp.int32), depth)


def by_columns(features, labels, weight, noise):
    coef = coefficients(features, labels, weight)
    partial_grad = lax.dot_general(
        features, coef, (((0,), (0,)), ((), ())), preferred_element_type=jnp.float32
    )
    classes = weight.shape[1] * lax.axis_size("cls")
    batch = features.shape[0] * lax.axis_size("ex")
    scale = 0.1 * classes / batch
    grad_part = lax.psum_scatter(partial_grad, "ex", scatter_dimension=0, tiled=True)
    span = grad_part.shape[0]
    own_weight = lax.dynamic_slice_in_dim(weight, lax.axis_index("ex") * span, span, 0)
    updated = own_weight.astype(jnp.float32) - scale * (
        grad_part + 0.96 * CLIP * noise.astype(jnp.float32)
    )
    return lax.all_gather(updated.astype(jnp.bfloat16), "ex", axis=0, tiled=True)


def local(features, labels, weight, noise):
    n = lax.axis_size("ex")
    layers = n // (2 * SIDES)
    fits = n % (2 * SIDES) == 0 and layers & (layers - 1) == 0 and layers > 1
    fits = fits and weight.shape[0] % (2 * SIDES * ROW) == 0 and weight.shape[0] % n == 0
    step = by_rows if fits else by_columns
    return step(features, labels, weight, noise)


def solution(mesh):
    in_specs = (P("ex", None), P("ex"), P(None, "cls"), P("ex", "cls"))
    out_specs = P(None, "cls")
    return jax.shard_map(local, mesh=mesh, in_specs=in_specs, out_specs=out_specs, check_vma=False)
```

```python
import jax
import jax.numpy as jnp
from jax import lax
from jax.experimental import pallas as pl
from jax.experimental.pallas import tpu as pltpu
from jax.sharding import PartitionSpec as P

CLIP = 48.0
SIDES = 4
ROW, LANE = 8, 128


def coefficients(features, labels, weight):
    cls_width = weight.shape[1]
    logits = jnp.dot(features, weight, preferred_element_type=jnp.float32)
    offset = lax.axis_index("cls") * cls_width
    local_lab = labels - offset
    columns = lax.broadcasted_iota(jnp.int32, (1, cls_width), 1)
    onehot = columns == local_lab[:, None]
    label_part = jnp.sum(jnp.where(onehot, logits, 0.0), axis=1)
    top = lax.pmax(jnp.max(logits, axis=1), "cls")
    expo = jnp.exp(logits - top[:, None])
    total, squares, label_logit = lax.psum(
        (jnp.sum(expo, axis=1), jnp.sum(expo * expo, axis=1), label_part), "cls"
    )
    probs = expo / total[:, None]
    label_prob = jnp.exp(label_logit - top) / total
    resid_sq = squares / (total * total) - 2.0 * label_prob + 1.0
    resid_norm = jnp.sqrt(jnp.maximum(resid_sq, 0.0))
    feat = features.astype(jnp.float32)
    feat_norm = jnp.sqrt(jnp.sum(feat * feat, axis=1))
    factor = CLIP / jnp.maximum(feat_norm * resid_norm, CLIP)
    resid = probs - onehot.astype(jnp.float32)
    return (factor[:, None] * resid).astype(jnp.bfloat16)


def copy_out(rows_ref, blocks, columns, out_ref, sems):
    copies = []
    for i, (block, first) in enumerate(zip(blocks, columns)):
        count, width = block.shape
        start = pl.multiple_of(rows_ref[i], ROW)
        place_at = out_ref.at[pl.ds(start, count), pl.ds(first, width)]
        copies.append(pltpu.make_async_copy(block, place_at, sems.at[i]))
    for copy in copies:
        copy.start()
    for copy in copies:
        copy.wait()


def place(blocks, rows, columns, shape, into=None):
    def kernel(rows_ref, *refs):
        out_ref, sems = refs[-2:]
        copy_out(rows_ref, refs[: len(blocks)], columns, out_ref, sems)

    where = pl.BlockSpec(memory_space=pl.ANY)
    extra = () if into is None else (into,)
    return pl.pallas_call(
        kernel,
        in_specs=[pl.BlockSpec(memory_space=pltpu.SMEM)]
        + [where] * (len(blocks) + len(extra)),
        out_specs=where,
        out_shape=jax.ShapeDtypeStruct(shape, blocks[0].dtype),
        scratch_shapes=[pltpu.SemaphoreType.DMA((len(blocks),))],
        input_output_aliases={len(blocks) + 1: 0} if extra else {},
        compiler_params=pltpu.CompilerParams(vmem_limit_bytes=1 << 20),
    )(jnp.stack(rows).astype(jnp.int32), *blocks, *extra)


def cut(total, pieces):
    own = total // pieces
    starts = [own * k // ROW * ROW for k in range(pieces)]
    window = max(-(-own * (k + 1) // ROW) * ROW - starts[k] for k in range(pieces))
    return [min(s, total - window) for s in starts], window


def rows_of(x, start, count):
    return lax.dynamic_slice_in_dim(x, start, count, 0)


def narrow_share(width):
    tiles = width // LANE
    return max(1, round(tiles * 4 / 11)) * LANE


class Ring:
    def __init__(self):
        n = self.n = lax.axis_size("ex")
        me = lax.axis_index("ex")
        self.layers = n // (2 * SIDES)
        self.core, self.layer = me % 2, me // (2 * SIDES)
        self.side = me // 2 % SIDES
        self.cores = [(i, i ^ 1) for i in range(n)]
        self.first = [(i, i ^ (4 if i % 2 else 2)) for i in range(n)]
        self.second = [(i, i ^ (2 if i % 2 else 4)) for i in range(n)]

    def swap(self, x, pairs):
        return lax.ppermute(x, "ex", pairs)

    def up(self, x, d):
        return self.swap(x, [(i, i ^ (2 * SIDES * d)) for i in range(self.n)])

    def side_at(self, far_first, far_second):
        flip_a = jnp.where(self.core == 0, far_first, far_second)
        flip_b = jnp.where(self.core == 0, far_second, far_first)
        return self.side ^ (flip_a + 2 * flip_b)

    def order_of_side(self, q):
        flip = self.side ^ q
        return jnp.where(self.core == 0, flip % 2 * 2 + flip // 2, flip)


def sum_sides(ring, x, starts, count):
    bf16, f32 = jnp.bfloat16, jnp.float32

    def at(a, b):
        return rows_of(x, starts[ring.side_at(a, b)], count)

    sent = jnp.concatenate([at(1, 1), at(1, 0)], axis=0).astype(bf16)
    got = ring.swap(sent, ring.first).astype(f32)
    passed = (at(0, 1) + got[:count]).astype(bf16)
    return at(0, 0) + got[count:] + ring.swap(passed, ring.second).astype(f32)


def sum_layers(ring, x, starts, count):
    bf16, f32 = jnp.bfloat16, jnp.float32
    total = rows_of(x, starts[ring.layer], count)
    for d in range(1, ring.layers):
        sent = rows_of(x, starts[ring.layer ^ d], count).astype(bf16)
        total = total + ring.up(sent, d).astype(f32)
    return total


def spread_sides(ring, x):
    second = ring.swap(x, ring.second)
    first = ring.swap(x, ring.first)
    return [x, second, first, ring.swap(second, ring.first)]


def spread_layers(ring, x):
    return [x] + [ring.up(x, d) for d in range(1, ring.layers)]


def join(parts, index_of, own, starts):
    ordered = []
    for k, start in enumerate(starts):
        which = jnp.broadcast_to(index_of(k), parts[0].shape)
        piece = lax.select_n(which.astype(jnp.int32), *parts)
        skip = own * k - start
        ordered.append(piece[skip : skip + own])
    return jnp.concatenate(ordered, axis=0)


def by_rows(features, labels, weight, noise):
    bf16, f32 = jnp.bfloat16, jnp.float32
    ring = Ring()
    n, layers = ring.n, ring.layers
    depth, width = weight.shape
    half, own = depth // 2, depth // n
    by_side, by_layer = half // SIDES, half // layers
    narrow = narrow_share(width)
    wide = width - narrow
    classes = width * lax.axis_size("cls")
    batch = features.shape[0] * n
    scale = 0.1 * classes / batch

    to_wide, to_narrow = [], []
    for d in range(n):
        c, rest = d // (SIDES * layers), d % (SIDES * layers)
        q, k = rest // layers, rest % layers
        to_wide.append((d, (k * SIDES + q) * 2 + c))
        k, q = rest // SIDES, rest % SIDES
        to_narrow.append((d, (k * SIDES + q) * 2 + c))
    noise_narrow = ring.swap(noise[:, wide:], to_narrow)
    noise_wide = ring.swap(noise[:, :wide], to_wide)

    def updated(grad, noise_own, base, start, inner, columns):
        count = grad.shape[0]
        noise_rows = lax.dynamic_update_slice_in_dim(
            jnp.zeros((count, grad.shape[1]), noise.dtype), noise_own, inner, 0
        )
        rows = lax.dynamic_slice(
            weight, (base + start, jnp.int32(columns)), (count, grad.shape[1])
        )
        return (
            rows.astype(f32) - scale * (grad + 0.96 * CLIP * noise_rows.astype(f32))
        ).astype(bf16)

    def core_sum(part):
        sent = rows_of(part, half * (1 - ring.core), half).astype(bf16)
        got = ring.swap(sent, ring.cores)
        return rows_of(part, half * ring.core, half) + got.astype(f32)

    coef = lax.optimization_barrier(coefficients(features, labels, weight))

    def gradient(columns):
        return lax.dot_general(
            features, columns, (((0,), (0,)), ((), ())), preferred_element_type=f32
        )

    side_rows = jnp.arange(SIDES, dtype=jnp.int32) * by_side
    layer_rows = jnp.arange(layers, dtype=jnp.int32) * by_layer
    wide_starts, wide_count = cut(by_side, layers)
    narrow_starts, narrow_count = cut(by_layer, SIDES)
    wide_table = jnp.asarray(wide_starts, jnp.int32)
    narrow_table = jnp.asarray(narrow_starts, jnp.int32)

    half_narrow = core_sum(gradient(coef[:, wide:]))
    half_wide = core_sum(gradient(coef[:, :wide]))
    layer_sum = sum_layers(ring, half_narrow, layer_rows, by_layer)
    side_sum = sum_sides(ring, half_wide, side_rows, by_side)
    grad_narrow = sum_sides(ring, layer_sum, narrow_table, narrow_count)
    grad_wide = sum_layers(ring, side_sum, wide_table, wide_count)

    start = narrow_table[ring.side]
    new_narrow = updated(
        grad_narrow,
        noise_narrow,
        half * ring.core + by_layer * ring.layer,
        start,
        own * ring.side - start,
        wide,
    )
    start = wide_table[ring.layer]
    new_wide = updated(
        grad_wide,
        noise_wide,
        half * ring.core + by_side * ring.side,
        start,
        own * ring.layer - start,
        0,
    )

    parts = spread_sides(ring, new_narrow)
    layer_block = join(parts, ring.order_of_side, own, narrow_starts)
    parts = spread_layers(ring, new_wide)
    side_block = join(parts, lambda k: ring.layer ^ k, own, wide_starts)
    narrow_blocks = spread_layers(ring, layer_block)
    wide_blocks = spread_sides(ring, side_block)

    narrow_rows = [by_layer * (ring.layer ^ d) for d in range(layers)]
    flips = [(0, 0), (0, 1), (1, 0), (1, 1)]
    wide_rows = [by_side * ring.side_at(a, b) for a, b in flips]
    other_rows = [by_side * ring.side_at(b, a) for a, b in flips]
    mine, theirs = half * ring.core, half * (1 - ring.core)
    blocks = narrow_blocks + wide_blocks
    far = [ring.swap(b, ring.cores) for b in blocks]
    columns = [wide] * layers + [0] * SIDES
    rows = [mine + r for r in narrow_rows + wide_rows]
    rows += [theirs + r for r in narrow_rows + other_rows]
    return place(blocks + far, rows, columns * 2, weight.shape)


def by_columns(features, labels, weight, noise):
    coef = coefficients(features, labels, weight)
    partial_grad = lax.dot_general(
        features, coef, (((0,), (0,)), ((), ())), preferred_element_type=jnp.float32
    )
    classes = weight.shape[1] * lax.axis_size("cls")
    batch = features.shape[0] * lax.axis_size("ex")
    scale = 0.1 * classes / batch
    grad_part = lax.psum_scatter(partial_grad, "ex", scatter_dimension=0, tiled=True)
    span = grad_part.shape[0]
    own_weight = lax.dynamic_slice_in_dim(weight, lax.axis_index("ex") * span, span, 0)
    updated = own_weight.astype(jnp.float32) - scale * (
        grad_part + 0.96 * CLIP * noise.astype(jnp.float32)
    )
    return lax.all_gather(updated.astype(jnp.bfloat16), "ex", axis=0, tiled=True)


def local(features, labels, weight, noise):
    n = lax.axis_size("ex")
    depth, width = weight.shape
    layers = n // (2 * SIDES)
    fits = n % (2 * SIDES) == 0 and layers > 1 and layers & (layers - 1) == 0
    fits = fits and depth % n == 0 and width % LANE == 0 and width > LANE
    fits = fits and depth % (2 * ROW * SIDES) == 0 and depth % (2 * ROW * layers) == 0
    step = by_rows if fits else by_columns
    return step(features, labels, weight, noise)


def solution(mesh):
    in_specs = (P("ex", None), P("ex"), P(None, "cls"), P("ex", "cls"))
    out_specs = P(None, "cls")
    return jax.shard_map(local, mesh=mesh, in_specs=in_specs, out_specs=out_specs, check_vma=False)
```

```python
import functools

import jax
import jax.numpy as jnp
from jax import lax
from jax.experimental import pallas as pl
from jax.experimental.pallas import tpu as pltpu
from jax.sharding import PartitionSpec as P


CLIP = 48.0
SIDES = 4
ROW, LANE = 8, 128


def coefficients(features, labels, weight):
    cls_width = weight.shape[1]
    logits = jnp.dot(features, weight, preferred_element_type=jnp.float32)
    offset = lax.axis_index("cls") * cls_width
    local_lab = labels - offset
    columns = lax.broadcasted_iota(jnp.int32, (1, cls_width), 1)
    onehot = columns == local_lab[:, None]
    label_part = jnp.sum(jnp.where(onehot, logits, 0.0), axis=1)
    top = lax.pmax(jnp.max(logits, axis=1), "cls")
    expo = jnp.exp(logits - top[:, None])
    total, squares, label_logit = lax.psum(
        (jnp.sum(expo, axis=1), jnp.sum(expo * expo, axis=1), label_part), "cls"
    )
    probs = expo / total[:, None]
    label_prob = jnp.exp(label_logit - top) / total
    resid_sq = squares / (total * total) - 2.0 * label_prob + 1.0
    resid_norm = jnp.sqrt(jnp.maximum(resid_sq, 0.0))
    feat = features.astype(jnp.float32)
    feat_norm = jnp.sqrt(jnp.sum(feat * feat, axis=1))
    factor = CLIP / jnp.maximum(feat_norm * resid_norm, CLIP)
    resid = probs - onehot.astype(jnp.float32)
    return (factor[:, None] * resid).astype(jnp.bfloat16)


def coefficient_rows(logits, rows, label):
    f32 = jnp.float32
    top = jnp.max(logits, axis=1, keepdims=True)
    expo = jnp.exp(logits - top)
    onehot = lax.broadcasted_iota(jnp.int32, logits.shape, 1) == label
    rest = jnp.where(onehot, 0.0, expo)
    total = jnp.sum(expo, axis=1, keepdims=True)
    others = jnp.sum(rest, axis=1, keepdims=True)
    squares = jnp.sum(rest * rest, axis=1, keepdims=True)
    feat = rows.astype(f32)
    feat_sq = jnp.sum(feat * feat, axis=1, keepdims=True)
    norm = jnp.sqrt(feat_sq) * jnp.sqrt(squares + others * others) / total
    gain = CLIP / jnp.maximum(norm, CLIP) / total
    return (jnp.where(onehot, -others, expo) * gain).astype(jnp.bfloat16)


def head_kernel(shape, core_ref, feat_ref, label_ref, weight_ref, *refs):
    block, part, slab, skip, columns, cuts = shape
    groups = len(columns)
    outs = refs[:groups], refs[groups : 2 * groups]
    feat, wgt, coef, even, odd, sent, kept, feat_sem, wgt_sem, out_sem = refs[2 * groups :]
    blocks = feat.shape[0] // block
    logits = even, odd

    def load_rows(i):
        at = pl.ds(i * block, block)
        return pltpu.make_async_copy(feat_ref.at[at], feat.at[at], feat_sem.at[i])

    def load_columns(i):
        at = pl.ds(cuts[i], cuts[i + 1] - cuts[i])
        return pltpu.make_async_copy(weight_ref.at[:, at], wgt.at[:, at], wgt_sem.at[i])

    load_rows(0).start()
    for i in range(len(cuts) - 1):
        load_columns(i).start()
    for i in range(1, blocks):
        load_rows(i).start()
    load_rows(0).wait()
    for i in range(len(cuts) - 1):
        load_columns(i).wait()
        even[:, cuts[i] : cuts[i + 1]] = jnp.dot(
            feat[:block, :], wgt[:, cuts[i] : cuts[i + 1]], preferred_element_type=jnp.float32
        )
    for i in range(1, blocks):
        load_rows(i).wait()

    def residuals(i):
        for j in range(block // part):
            r = i * block + j * part
            line = label_ref[r // LANE : r // LANE + 1, :]
            label = jnp.broadcast_to(line, (LANE, LANE)).T[:, :1]
            coef[r : r + part, :] = coefficient_rows(
                logits[i % 2][j * part : (j + 1) * part, :], feat[r : r + part, :], label
            )

    for i in range(1, blocks):
        logits[i % 2][...] = jnp.dot(
            feat[i * block : (i + 1) * block, :], wgt[...], preferred_element_type=jnp.float32
        )
        residuals(i - 1)
    residuals(blocks - 1)

    tiles = slab // LANE
    copies = []
    for side, buf in enumerate((sent, kept)):
        which = core_ref[0] if side else 1 - core_ref[0]
        base = which * (feat_ref.shape[1] - slab)
        for m in range(tiles):
            off = pl.multiple_of(base + m * LANE, LANE)
            buf[m * LANE : (m + 1) * LANE, :] = lax.dot_general(
                feat[:, pl.ds(off, LANE)],
                coef[...],
                (((0,), (0,)), ((), ())),
                preferred_element_type=jnp.float32,
            ).astype(buf.dtype)
            low, high = max(0, m * LANE - skip), (m + 1) * LANE - skip
            source = pl.ds(pl.multiple_of(which * skip + low, ROW), high - low)
            for g, (first, width) in enumerate(columns):
                copies.append(
                    pltpu.make_async_copy(
                        buf.at[source, pl.ds(first, width)],
                        outs[side][g].at[pl.ds(low, high - low)],
                        out_sem.at[len(copies)],
                    )
                )
                copies[-1].start()
    for copy in copies:
        copy.wait()


def halves(features, labels, weight, core, columns):
    n, depth = features.shape
    width = weight.shape[1]
    half = depth // 2
    slab = -(-half // LANE) * LANE
    bf16, f32 = jnp.bfloat16, jnp.float32
    block = 2 * LANE if n % (2 * LANE) == 0 else LANE
    chunks = min(4, width // LANE)
    cuts = [round(width // LANE * i / chunks) * LANE for i in range(chunks + 1)]
    shape = block, LANE, slab, slab - half, columns, cuts
    anywhere = pl.BlockSpec(memory_space=pl.ANY)
    return pl.pallas_call(
        functools.partial(head_kernel, shape),
        in_specs=[
            pl.BlockSpec(memory_space=pltpu.SMEM),
            anywhere,
            pl.BlockSpec(memory_space=pltpu.VMEM),
            anywhere,
        ],
        out_specs=[anywhere] * (2 * len(columns)),
        out_shape=[jax.ShapeDtypeStruct((half, w), bf16) for _, w in columns]
        + [jax.ShapeDtypeStruct((half, w), f32) for _, w in columns],
        scratch_shapes=[
            pltpu.VMEM((n, depth), bf16),
            pltpu.VMEM((depth, width), bf16),
            pltpu.VMEM((n, width), bf16),
            pltpu.VMEM((block, width), f32),
            pltpu.VMEM((block, width), f32),
            pltpu.VMEM((slab, width), bf16),
            pltpu.VMEM((slab, width), f32),
            pltpu.SemaphoreType.DMA((n // block,)),
            pltpu.SemaphoreType.DMA((chunks,)),
            pltpu.SemaphoreType.DMA((2 * slab // LANE * len(columns),)),
        ],
        compiler_params=pltpu.CompilerParams(vmem_limit_bytes=60 << 20),
        cost_estimate=pl.CostEstimate(
            flops=4 * n * depth * width,
            bytes_accessed=2 * n * depth + 5 * depth * width,
            transcendentals=n * width,
        ),
        name="halves",
    )(core.reshape(1), features, labels.reshape(n // LANE, LANE), weight)


def place(blocks, rows, columns, shape, into=None):
    count = len(blocks)

    def kernel(rows_ref, *refs):
        out_ref = refs[-count - 3]
        held, load_sem, save_sem = refs[-count - 2 : -2], refs[-2], refs[-1]
        loads, saves = [], []
        for i in range(count):
            start = pl.multiple_of(rows_ref[i], ROW)
            at = out_ref.at[pl.ds(start, blocks[i].shape[0]), pl.ds(columns[i], blocks[i].shape[1])]
            loads.append(pltpu.make_async_copy(refs[i], held[i], load_sem.at[i]))
            saves.append(pltpu.make_async_copy(held[i], at, save_sem.at[i]))
        for load in loads:
            load.start()
        for load, save in zip(loads, saves):
            load.wait()
            save.start()
        for save in saves:
            save.wait()

    extra = () if into is None else (into,)
    anywhere = pl.BlockSpec(memory_space=pl.ANY)
    return pl.pallas_call(
        kernel,
        in_specs=[pl.BlockSpec(memory_space=pltpu.SMEM)] + [anywhere] * (count + len(extra)),
        out_specs=anywhere,
        out_shape=jax.ShapeDtypeStruct(shape, blocks[0].dtype),
        scratch_shapes=[pltpu.VMEM(b.shape, b.dtype) for b in blocks]
        + [pltpu.SemaphoreType.DMA((count,)), pltpu.SemaphoreType.DMA((count,))],
        input_output_aliases={count + 1: 0} if extra else {},
        compiler_params=pltpu.CompilerParams(vmem_limit_bytes=16 << 20),
        name="place",
    )(jnp.stack(rows).astype(jnp.int32), *blocks, *extra)


def cut(total, pieces):
    own = total // pieces
    starts = [own * k // ROW * ROW for k in range(pieces)]
    window = max(-(-own * (k + 1) // ROW) * ROW - starts[k] for k in range(pieces))
    return [min(s, total - window) for s in starts], window


def rows_of(x, start, count):
    return lax.dynamic_slice_in_dim(x, start, count, 0)


def narrow_share(width):
    tiles = width // LANE
    return max(1, round(tiles * 4 / 11)) * LANE


class Group:
    def __init__(self, stride, count):
        n = lax.axis_size("ex")
        self.count = count
        self.index = lax.axis_index("ex") // stride % count
        self.pairs = [[(i, i ^ (stride * d)) for i in range(n)] for d in range(count)]

    def swap(self, x, d):
        return lax.ppermute(x, "ex", self.pairs[d])

    def sum(self, rows_at, starts):
        got = []
        for d in range(1, self.count):
            sent = rows_at(starts[self.index ^ d]).astype(jnp.bfloat16)
            got.append(self.swap(sent, d))
        total = rows_at(starts[self.index])
        for part in got:
            total = total + part.astype(jnp.float32)
        return total

    def spread(self, x):
        return [x] + [self.swap(x, d) for d in range(1, self.count)]


def two_way(core):
    return [jnp.where(core == 0, 2, 1), jnp.where(core == 0, 1, 2), 3]


def two_way_swaps():
    n = lax.axis_size("ex")
    first = [(i, i ^ (4 if i % 2 else 2)) for i in range(n)]
    second = [(i, i ^ (2 if i % 2 else 4)) for i in range(n)]
    return first, second


def two_way_sum(core, side, rows_at, starts):
    bf16, f32 = jnp.bfloat16, jnp.float32
    first, second = two_way_swaps()
    second_d, first_d, far_d = two_way(core)

    def at(d):
        return rows_at(starts[side.index ^ d])

    sent = jnp.concatenate([at(far_d).astype(bf16), at(first_d).astype(bf16)], axis=0)
    got = lax.ppermute(sent, "ex", first)
    count = sent.shape[0] // 2
    passed = (at(second_d) + got[:count].astype(f32)).astype(bf16)
    last = lax.ppermute(passed, "ex", second)
    return at(0) + got[count:].astype(f32) + last.astype(f32)


def two_way_spread(x, out):
    first, second = two_way_swaps()
    from_second = lax.ppermute(x, "ex", second)
    from_first = lax.ppermute(x, "ex", first)
    from_second, out = lax.optimization_barrier((from_second, out))
    far = lax.ppermute(from_second, "ex", first)
    return [from_second, from_first, far], out


def join(parts, index, own, starts):
    ordered = []
    for k, start in enumerate(starts):
        which = jnp.broadcast_to(index ^ k, parts[0].shape)
        piece = lax.select_n(which.astype(jnp.int32), *parts)
        skip = own * k - start
        ordered.append(piece[skip : skip + own])
    return jnp.concatenate(ordered, axis=0)


def by_rows(features, labels, weight, noise):
    bf16, f32 = jnp.bfloat16, jnp.float32
    n = lax.axis_size("ex")
    layers = n // (2 * SIDES)
    core, side, layer = Group(1, 2), Group(2, SIDES), Group(2 * SIDES, layers)
    depth, width = weight.shape
    half, own = depth // 2, depth // n
    by_side, by_layer = half // SIDES, half // layers
    narrow = narrow_share(width)
    wide = width - narrow
    classes = width * lax.axis_size("cls")
    batch = features.shape[0] * n
    scale = 0.1 * classes / batch

    to_wide, to_narrow = [], []
    for d in range(n):
        c, rest = d // (SIDES * layers), d % (SIDES * layers)
        q, k = rest // layers, rest % layers
        to_wide.append((d, (k * SIDES + q) * 2 + c))
        k, q = rest // SIDES, rest % SIDES
        to_narrow.append((d, (k * SIDES + q) * 2 + c))

    def shifted(noise_own, starts, index):
        count = wide_count if starts is wide_starts else narrow_count
        shapes = []
        for k, start in enumerate(starts):
            skip = own * k - start
            shapes.append(jnp.pad(noise_own, ((skip, count - own - skip), (0, 0))))
        which = jnp.broadcast_to(index, shapes[0].shape)
        return lax.select_n(which.astype(jnp.int32), *shapes)

    def updated(grad, noise_rows, begin, columns):
        rows = lax.dynamic_slice(weight, (begin, jnp.int32(columns)), grad.shape)
        return (
            rows.astype(f32) - scale * (grad + 0.96 * CLIP * noise_rows.astype(f32))
        ).astype(bf16)

    columns = [(wide, narrow), (0, wide)]
    if lax.axis_size("cls") == 1 and features.shape[0] % LANE == 0:
        sent_n, sent_w, kept_n, kept_w = halves(
            features, labels, weight, core.index, columns
        )
    else:
        coef = coefficients(features, labels, weight)
        grad = lax.dot_general(
            features, coef, (((0,), (0,)), ((), ())), preferred_element_type=f32
        )
        sent = rows_of(grad, half * (1 - core.index), half).astype(bf16)
        kept = rows_of(grad, half * core.index, half)
        sent_n, sent_w = sent[:, wide:], sent[:, :wide]
        kept_n, kept_w = kept[:, wide:], kept[:, :wide]

    side_rows = jnp.arange(SIDES, dtype=jnp.int32) * by_side
    layer_rows = jnp.arange(layers, dtype=jnp.int32) * by_layer
    wide_starts, wide_count = cut(by_side, layers)
    narrow_starts, narrow_count = cut(by_layer, SIDES)
    wide_table = jnp.asarray(wide_starts, jnp.int32)
    narrow_table = jnp.asarray(narrow_starts, jnp.int32)

    got_n, got_w = core.swap(sent_n, 1), core.swap(sent_w, 1)
    noise, kept_n, kept_w = lax.optimization_barrier((noise, kept_n, kept_w))
    noise_n = lax.ppermute(noise[:, wide:], "ex", to_narrow)
    noise_w = lax.ppermute(noise[:, :wide], "ex", to_wide)

    def narrow_rows(start):
        return rows_of(kept_n, start, by_layer) + rows_of(got_n, start, by_layer).astype(f32)

    def wide_rows(start):
        return rows_of(kept_w, start, by_side) + rows_of(got_w, start, by_side).astype(f32)

    layer_sum = layer.sum(narrow_rows, layer_rows)
    side_sum = two_way_sum(core.index, side, wide_rows, side_rows)
    noise_n = shifted(noise_n, narrow_starts, side.index)
    noise_w = shifted(noise_w, wide_starts, layer.index)
    layer_sum, side_sum, noise_n, noise_w = lax.optimization_barrier(
        (layer_sum, side_sum, noise_n, noise_w)
    )
    grad_n = side.sum(lambda start: rows_of(layer_sum, start, narrow_count), narrow_table)
    grad_w = layer.sum(lambda start: rows_of(side_sum, start, wide_count), wide_table)

    begin = half * core.index + by_layer * layer.index + narrow_table[side.index]
    new_narrow = updated(grad_n, noise_n, begin, wide)
    begin = half * core.index + by_side * side.index + wide_table[layer.index]
    new_wide = updated(grad_w, noise_w, begin, 0)
    new_narrow, new_wide = lax.optimization_barrier((new_narrow, new_wide))
    layer_parts, side_parts = lax.optimization_barrier(
        (side.spread(new_narrow), layer.spread(new_wide))
    )
    layer_block = join(layer_parts, side.index, own, narrow_starts)
    side_block = join(side_parts, layer.index, own, wide_starts)
    near = [layer_block, side_block]
    near += [core.swap(b, 1) for b in near]
    mine, other = half * core.index, half * (1 - core.index)
    narrow_at = [by_layer * (layer.index ^ d) for d in range(layers)]
    wide_at = [by_side * (side.index ^ d) for d in range(SIDES)]
    rows = [mine + narrow_at[0], mine + wide_at[0], other + narrow_at[0], other + wide_at[0]]
    out = place(near, rows, [wide, 0] * 2, weight.shape)

    blocks = layer.spread(layer_block)[1:]
    side_blocks, out = two_way_spread(side_block, out)
    side_rows = [mine + by_side * (side.index ^ d) for d in two_way(core.index)]
    side_blocks += [core.swap(b, 1) for b in side_blocks]
    side_rows += [other + by_side * (side.index ^ d) for d in two_way(1 - core.index)]
    early = [0, 1, 3, 4]
    out = place(
        [side_blocks[i] for i in early], [side_rows[i] for i in early], [0] * 4, weight.shape, out
    )
    blocks += [core.swap(b, 1) for b in blocks]
    rows = [mine + r for r in narrow_at[1:]] + [other + r for r in narrow_at[1:]]
    columns = [wide] * len(rows) + [0] * 2
    return place(
        blocks + [side_blocks[2], side_blocks[5]],
        rows + [side_rows[2], side_rows[5]],
        columns,
        weight.shape,
        out,
    )


def by_columns(features, labels, weight, noise):
    coef = coefficients(features, labels, weight)
    partial_grad = lax.dot_general(
        features, coef, (((0,), (0,)), ((), ())), preferred_element_type=jnp.float32
    )
    classes = weight.shape[1] * lax.axis_size("cls")
    batch = features.shape[0] * lax.axis_size("ex")
    scale = 0.1 * classes / batch
    grad_part = lax.psum_scatter(partial_grad, "ex", scatter_dimension=0, tiled=True)
    span = grad_part.shape[0]
    own_weight = lax.dynamic_slice_in_dim(weight, lax.axis_index("ex") * span, span, 0)
    updated = own_weight.astype(jnp.float32) - scale * (
        grad_part + 0.96 * CLIP * noise.astype(jnp.float32)
    )
    return lax.all_gather(updated.astype(jnp.bfloat16), "ex", axis=0, tiled=True)


def local(features, labels, weight, noise):
    n = lax.axis_size("ex")
    depth, width = weight.shape
    layers = n // (2 * SIDES)
    fits = n % (2 * SIDES) == 0 and layers > 1 and layers & (layers - 1) == 0
    fits = fits and depth % n == 0 and width % LANE == 0 and width > LANE
    fits = fits and depth % (2 * ROW * SIDES) == 0 and depth % (2 * ROW * layers) == 0
    if not fits:
        return by_columns(features, labels, weight, noise)
    return by_rows(features, labels, weight, noise)


def solution(mesh):
    in_specs = (P("ex", None), P("ex"), P(None, "cls"), P("ex", "cls"))
    out_specs = P(None, "cls")
    return jax.shard_map(
        local, mesh=mesh, in_specs=in_specs, out_specs=out_specs, check_vma=False
    )
```

```python
import functools

import jax
import jax.numpy as jnp
from jax import lax
from jax.experimental import pallas as pl
from jax.experimental.pallas import tpu as pltpu
from jax.sharding import PartitionSpec as P


CLIP = 48.0
SIDES = 4
ROW, LANE = 8, 128


def coefficients(features, labels, weight):
    cls_width = weight.shape[1]
    logits = jnp.dot(features, weight, preferred_element_type=jnp.float32)
    offset = lax.axis_index("cls") * cls_width
    local_lab = labels - offset
    columns = lax.broadcasted_iota(jnp.int32, (1, cls_width), 1)
    onehot = columns == local_lab[:, None]
    label_part = jnp.sum(jnp.where(onehot, logits, 0.0), axis=1)
    top = lax.pmax(jnp.max(logits, axis=1), "cls")
    expo = jnp.exp(logits - top[:, None])
    total, squares, label_logit = lax.psum(
        (jnp.sum(expo, axis=1), jnp.sum(expo * expo, axis=1), label_part), "cls"
    )
    probs = expo / total[:, None]
    label_prob = jnp.exp(label_logit - top) / total
    resid_sq = squares / (total * total) - 2.0 * label_prob + 1.0
    resid_norm = jnp.sqrt(jnp.maximum(resid_sq, 0.0))
    feat = features.astype(jnp.float32)
    feat_norm = jnp.sqrt(jnp.sum(feat * feat, axis=1))
    factor = CLIP / jnp.maximum(feat_norm * resid_norm, CLIP)
    resid = probs - onehot.astype(jnp.float32)
    return (factor[:, None] * resid).astype(jnp.bfloat16)


def coefficient_rows(logits, rows, label):
    f32 = jnp.float32
    top = jnp.max(logits, axis=1, keepdims=True)
    expo = jnp.exp(logits - top)
    onehot = lax.broadcasted_iota(jnp.int32, logits.shape, 1) == label
    rest = jnp.where(onehot, 0.0, expo)
    total = jnp.sum(expo, axis=1, keepdims=True)
    others = jnp.sum(rest, axis=1, keepdims=True)
    squares = jnp.sum(rest * rest, axis=1, keepdims=True)
    feat = rows.astype(f32)
    feat_sq = jnp.sum(feat * feat, axis=1, keepdims=True)
    norm = jnp.sqrt(feat_sq) * jnp.sqrt(squares + others * others) / total
    gain = CLIP / jnp.maximum(norm, CLIP) / total
    return (jnp.where(onehot, -others, expo) * gain).astype(jnp.bfloat16)


def head_kernel(shape, feat_ref, label_ref, weight_ref, *refs):
    block, part, slab, skip, columns, cuts = shape
    groups = len(columns)
    outs = refs[:groups], refs[groups : 2 * groups]
    feat, wgt, coef, even, odd, sent, kept, feat_sem, wgt_sem, out_sem = refs[2 * groups :]
    blocks = feat.shape[0] // block
    logits = even, odd

    def load_rows(i):
        at = pl.ds(i * block, block)
        return pltpu.make_async_copy(feat_ref.at[at], feat.at[at], feat_sem.at[i])

    def load_columns(i):
        at = pl.ds(cuts[i], cuts[i + 1] - cuts[i])
        return pltpu.make_async_copy(weight_ref.at[:, at], wgt.at[:, at], wgt_sem.at[i])

    load_rows(0).start()
    for i in range(len(cuts) - 1):
        load_columns(i).start()
    for i in range(1, blocks):
        load_rows(i).start()
    load_rows(0).wait()
    for i in range(len(cuts) - 1):
        load_columns(i).wait()
        even[:, cuts[i] : cuts[i + 1]] = jnp.dot(
            feat[:block, :], wgt[:, cuts[i] : cuts[i + 1]], preferred_element_type=jnp.float32
        )
    for i in range(1, blocks):
        load_rows(i).wait()

    def residuals(i):
        for j in range(block // part):
            r = i * block + j * part
            line = label_ref[r // LANE : r // LANE + 1, :]
            label = jnp.broadcast_to(line, (LANE, LANE)).T[:, :1]
            coef[r : r + part, :] = coefficient_rows(
                logits[i % 2][j * part : (j + 1) * part, :], feat[r : r + part, :], label
            )

    for i in range(1, blocks):
        logits[i % 2][...] = jnp.dot(
            feat[i * block : (i + 1) * block, :], wgt[...], preferred_element_type=jnp.float32
        )
        residuals(i - 1)
    residuals(blocks - 1)

    tiles = slab // LANE
    copies = []
    for side, buf in enumerate((sent, kept)):
        core = lax.axis_index("ex") % 2
        which = core if side else 1 - core
        base = which * (feat_ref.shape[1] - slab)
        for m in range(tiles):
            off = pl.multiple_of(base + m * LANE, LANE)
            buf[m * LANE : (m + 1) * LANE, :] = lax.dot_general(
                feat[:, pl.ds(off, LANE)],
                coef[...],
                (((0,), (0,)), ((), ())),
                preferred_element_type=jnp.float32,
            ).astype(buf.dtype)
            low, high = max(0, m * LANE - skip), (m + 1) * LANE - skip
            source = pl.ds(pl.multiple_of(which * skip + low, ROW), high - low)
            for g, (first, width) in enumerate(columns):
                copies.append(
                    pltpu.make_async_copy(
                        buf.at[source, pl.ds(first, width)],
                        outs[side][g].at[pl.ds(low, high - low)],
                        out_sem.at[len(copies)],
                    )
                )
                copies[-1].start()
    for copy in copies:
        copy.wait()


def halves(features, labels, weight, columns):
    n, depth = features.shape
    width = weight.shape[1]
    half = depth // 2
    slab = -(-half // LANE) * LANE
    bf16, f32 = jnp.bfloat16, jnp.float32
    block = 2 * LANE if n % (2 * LANE) == 0 else LANE
    chunks = min(4, width // LANE)
    cuts = [round(width // LANE * i / chunks) * LANE for i in range(chunks + 1)]
    shape = block, LANE, slab, slab - half, columns, cuts
    anywhere = pl.BlockSpec(memory_space=pl.ANY)
    return pl.pallas_call(
        functools.partial(head_kernel, shape),
        in_specs=[anywhere, pl.BlockSpec(memory_space=pltpu.VMEM), anywhere],
        out_specs=[anywhere] * (2 * len(columns)),
        out_shape=[jax.ShapeDtypeStruct((half, w), bf16) for _, w in columns]
        + [jax.ShapeDtypeStruct((half, w), f32) for _, w in columns],
        scratch_shapes=[
            pltpu.VMEM((n, depth), bf16),
            pltpu.VMEM((depth, width), bf16),
            pltpu.VMEM((n, width), bf16),
            pltpu.VMEM((block, width), f32),
            pltpu.VMEM((block, width), f32),
            pltpu.VMEM((slab, width), bf16),
            pltpu.VMEM((slab, width), f32),
            pltpu.SemaphoreType.DMA((n // block,)),
            pltpu.SemaphoreType.DMA((chunks,)),
            pltpu.SemaphoreType.DMA((2 * slab // LANE * len(columns),)),
        ],
        compiler_params=pltpu.CompilerParams(vmem_limit_bytes=60 << 20),
        cost_estimate=pl.CostEstimate(
            flops=4 * n * depth * width,
            bytes_accessed=2 * n * depth + 5 * depth * width,
            transcendentals=n * width,
        ),
        name="halves",
    )(features, labels.reshape(n // LANE, LANE), weight)


def place(blocks, rows, columns, shape, into=None):
    count = len(blocks)

    def kernel(*refs):
        firsts = rows()
        out_ref = refs[-count - 3]
        held, load_sem, save_sem = refs[-count - 2 : -2], refs[-2], refs[-1]
        loads, saves = [], []
        for i in range(count):
            start = pl.multiple_of(firsts[i], ROW)
            at = out_ref.at[pl.ds(start, blocks[i].shape[0]), pl.ds(columns[i], blocks[i].shape[1])]
            loads.append(pltpu.make_async_copy(refs[i], held[i], load_sem.at[i]))
            saves.append(pltpu.make_async_copy(held[i], at, save_sem.at[i]))
        for load in loads:
            load.start()
        for load, save in zip(loads, saves):
            load.wait()
            save.start()
        for save in saves:
            save.wait()

    extra = () if into is None else (into,)
    anywhere = pl.BlockSpec(memory_space=pl.ANY)
    return pl.pallas_call(
        kernel,
        in_specs=[anywhere] * (count + len(extra)),
        out_specs=anywhere,
        out_shape=jax.ShapeDtypeStruct(shape, blocks[0].dtype),
        scratch_shapes=[pltpu.VMEM(b.shape, b.dtype) for b in blocks]
        + [pltpu.SemaphoreType.DMA((count,)), pltpu.SemaphoreType.DMA((count,))],
        input_output_aliases={count: 0} if extra else {},
        compiler_params=pltpu.CompilerParams(vmem_limit_bytes=16 << 20),
        name="place",
    )(*blocks, *extra)


class Cut:
    def __init__(self, total, pieces):
        self.own, self.pieces = total // pieces, pieces
        firsts = [self.own * k // ROW * ROW for k in range(pieces)]
        lasts = [-(-self.own * (k + 1) // ROW) * ROW for k in range(pieces)]
        self.count = max(last - first for first, last in zip(firsts, lasts))
        self.most = total - self.count
        self.skips = [self.own * k - min(f, self.most) for k, f in enumerate(firsts)]

    def start(self, k):
        first = self.own * k
        return lax.min(first - lax.rem(first, ROW), jnp.int32(self.most))


def rows_of(x, start, count):
    return lax.dynamic_slice_in_dim(x, start, count, 0)


def narrow_share(width):
    tiles = width // LANE
    return max(1, round(tiles * 4 / 11)) * LANE


class Group:
    def __init__(self, stride, count):
        n = lax.axis_size("ex")
        self.count = count
        self.index = lax.axis_index("ex") // stride % count
        self.pairs = [[(i, i ^ (stride * d)) for i in range(n)] for d in range(count)]

    def swap(self, x, d):
        return lax.ppermute(x, "ex", self.pairs[d])

    def sum(self, rows_at):
        got = []
        for d in reversed(range(1, self.count)):
            sent = rows_at(self.index ^ d).astype(jnp.bfloat16)
            got.append(self.swap(sent, d))
        total = rows_at(self.index)
        for part in got:
            total = total + part.astype(jnp.float32)
        return total

    def spread(self, x):
        return [x] + [self.swap(x, d) for d in range(1, self.count)]


def two_way(core):
    return [jnp.where(core == 0, 2, 1), jnp.where(core == 0, 1, 2), 3]


def two_way_swaps():
    n = lax.axis_size("ex")
    first = [(i, i ^ (4 if i % 2 else 2)) for i in range(n)]
    second = [(i, i ^ (2 if i % 2 else 4)) for i in range(n)]
    return first, second


def two_way_sum(core, side, rows_at):
    bf16, f32 = jnp.bfloat16, jnp.float32
    first, second = two_way_swaps()
    second_d, first_d, far_d = two_way(core)

    def at(d):
        return rows_at(side.index ^ d)

    sent = jnp.concatenate([at(far_d).astype(bf16), at(first_d).astype(bf16)], axis=0)
    got = lax.ppermute(sent, "ex", first)
    count = sent.shape[0] // 2
    passed = (at(second_d) + got[:count].astype(f32)).astype(bf16)
    last = lax.ppermute(passed, "ex", second)
    return at(0) + got[count:].astype(f32) + last.astype(f32)


def two_way_spread(x):
    first, second = two_way_swaps()
    from_second = lax.ppermute(x, "ex", second)
    from_first = lax.ppermute(x, "ex", first)
    far = lax.ppermute(from_second, "ex", first)
    return [from_second, from_first, far]


def join(parts, index, cut):
    ordered = []
    for k, skip in enumerate(cut.skips):
        which = jnp.broadcast_to(index ^ k, parts[0].shape)
        piece = lax.select_n(which.astype(jnp.int32), *parts)
        ordered.append(piece[skip : skip + cut.own])
    return jnp.concatenate(ordered, axis=0)


def by_rows(features, labels, weight, noise):
    bf16, f32 = jnp.bfloat16, jnp.float32
    n = lax.axis_size("ex")
    layers = n // (2 * SIDES)
    core, side, layer = Group(1, 2), Group(2, SIDES), Group(2 * SIDES, layers)
    depth, width = weight.shape
    half, own = depth // 2, depth // n
    by_side, by_layer = half // SIDES, half // layers
    narrow = narrow_share(width)
    wide = width - narrow
    classes = width * lax.axis_size("cls")
    batch = features.shape[0] * n
    scale = 0.1 * classes / batch

    to_wide, to_narrow = [], []
    for d in range(n):
        c, rest = d // (SIDES * layers), d % (SIDES * layers)
        q, k = rest // layers, rest % layers
        to_wide.append((d, (k * SIDES + q) * 2 + c))
        k, q = rest // SIDES, rest % SIDES
        to_narrow.append((d, (k * SIDES + q) * 2 + c))

    wide_cut, narrow_cut = Cut(by_side, layers), Cut(by_layer, SIDES)

    def shifted(noise_own, cut, index):
        shapes = []
        for skip in cut.skips:
            shapes.append(jnp.pad(noise_own, ((skip, cut.count - own - skip), (0, 0))))
        which = jnp.broadcast_to(index, shapes[0].shape)
        return lax.select_n(which.astype(jnp.int32), *shapes)

    def updated(grad, noise_rows, begin, columns):
        rows = lax.dynamic_slice(weight, (begin, jnp.int32(columns)), grad.shape)
        return (
            rows.astype(f32) - scale * (grad + 0.96 * CLIP * noise_rows.astype(f32))
        ).astype(bf16)

    columns = [(wide, narrow), (0, wide)]
    if lax.axis_size("cls") == 1 and features.shape[0] % LANE == 0:
        sent_n, sent_w, kept_n, kept_w = halves(
            features, labels, weight, columns
        )
    else:
        coef = coefficients(features, labels, weight)
        grad = lax.dot_general(
            features, coef, (((0,), (0,)), ((), ())), preferred_element_type=f32
        )
        sent = rows_of(grad, half * (1 - core.index), half).astype(bf16)
        kept = rows_of(grad, half * core.index, half)
        sent_n, sent_w = sent[:, wide:], sent[:, :wide]
        kept_n, kept_w = kept[:, wide:], kept[:, :wide]

    got_n = core.swap(sent_n, 1)
    got_w = core.swap(sent_w, 1)
    noise, kept_n, kept_w = lax.optimization_barrier((noise, kept_n, kept_w))
    noise_n = lax.ppermute(noise[:, wide:], "ex", to_narrow)
    noise_w = lax.ppermute(noise[:, :wide], "ex", to_wide)

    def narrow_rows(k):
        start = by_layer * k
        return rows_of(kept_n, start, by_layer) + rows_of(got_n, start, by_layer).astype(f32)

    def wide_rows(k):
        start = by_side * k
        return rows_of(kept_w, start, by_side) + rows_of(got_w, start, by_side).astype(f32)

    layer_sum = layer.sum(narrow_rows)
    side_sum = two_way_sum(core.index, side, wide_rows)
    layer_sum, side_sum = lax.optimization_barrier((layer_sum, side_sum))
    noise_n = shifted(noise_n, narrow_cut, side.index)
    noise_w = shifted(noise_w, wide_cut, layer.index)
    noise_n, noise_w = lax.optimization_barrier((noise_n, noise_w))
    grad_n = side.sum(lambda k: rows_of(layer_sum, narrow_cut.start(k), narrow_cut.count))
    grad_w = layer.sum(lambda k: rows_of(side_sum, wide_cut.start(k), wide_cut.count))

    begin = half * core.index + by_layer * layer.index + narrow_cut.start(side.index)
    new_narrow = updated(grad_n, noise_n, begin, wide)
    begin = half * core.index + by_side * side.index + wide_cut.start(layer.index)
    new_wide = updated(grad_w, noise_w, begin, 0)
    new_narrow, new_wide = lax.optimization_barrier((new_narrow, new_wide))
    layer_parts, side_parts = lax.optimization_barrier(
        (side.spread(new_narrow), layer.spread(new_wide))
    )
    layer_block = join(layer_parts, side.index, narrow_cut)
    side_block = join(side_parts, layer.index, wide_cut)
    near = [layer_block, side_block]
    near += [core.swap(b, 1) for b in near]

    def rows_in(of_core):
        def rows():
            at = lax.axis_index("ex")
            c = at % 2 if of_core == 0 else 1 - at % 2
            q, k = at // 2 % SIDES, at // (2 * SIDES)
            narrow_at = [half * c + by_layer * (k ^ d) for d in range(layers)]
            wide_at = [half * c + by_side * (q ^ d) for d in [0] + two_way(c)]
            return narrow_at, wide_at

        return rows

    def near_rows():
        (a, b), (c, d) = rows_in(0)(), rows_in(1)()
        return [a[0], b[0], c[0], d[0]]

    def early_rows():
        (_, b), (_, d) = rows_in(0)(), rows_in(1)()
        return b[1:3] + d[1:3]

    def late_rows():
        (a, b), (c, d) = rows_in(0)(), rows_in(1)()
        return a[1:] + c[1:] + [b[3], d[3]]

    out = place(near, near_rows, [wide, 0] * 2, weight.shape)

    blocks = layer.spread(layer_block)[1:]
    side_blocks = two_way_spread(side_block)
    side_blocks += [core.swap(b, 1) for b in side_blocks]
    early = [side_blocks[i] for i in (0, 1, 3, 4)]
    out = place(early, early_rows, [0] * 4, weight.shape, out)
    blocks += [core.swap(b, 1) for b in blocks]
    columns = [wide] * len(blocks) + [0] * 2
    blocks += [side_blocks[2], side_blocks[5]]
    return place(blocks, late_rows, columns, weight.shape, out)


def by_columns(features, labels, weight, noise):
    coef = coefficients(features, labels, weight)
    partial_grad = lax.dot_general(
        features, coef, (((0,), (0,)), ((), ())), preferred_element_type=jnp.float32
    )
    classes = weight.shape[1] * lax.axis_size("cls")
    batch = features.shape[0] * lax.axis_size("ex")
    scale = 0.1 * classes / batch
    grad_part = lax.psum_scatter(partial_grad, "ex", scatter_dimension=0, tiled=True)
    span = grad_part.shape[0]
    own_weight = lax.dynamic_slice_in_dim(weight, lax.axis_index("ex") * span, span, 0)
    updated = own_weight.astype(jnp.float32) - scale * (
        grad_part + 0.96 * CLIP * noise.astype(jnp.float32)
    )
    return lax.all_gather(updated.astype(jnp.bfloat16), "ex", axis=0, tiled=True)


def local(features, labels, weight, noise):
    n = lax.axis_size("ex")
    depth, width = weight.shape
    layers = n // (2 * SIDES)
    fits = n % (2 * SIDES) == 0 and layers > 1 and layers & (layers - 1) == 0
    fits = fits and depth % n == 0 and width % LANE == 0 and width > LANE
    fits = fits and depth % (2 * ROW * SIDES) == 0 and depth % (2 * ROW * layers) == 0
    if not fits:
        return by_columns(features, labels, weight, noise)
    return by_rows(features, labels, weight, noise)


def solution(mesh):
    in_specs = (P("ex", None), P("ex"), P(None, "cls"), P("ex", "cls"))
    out_specs = P(None, "cls")
    return jax.shard_map(
        local, mesh=mesh, in_specs=in_specs, out_specs=out_specs, check_vma=False
    )
```

```python
import functools

import jax
import jax.numpy as jnp
from jax import lax
from jax.experimental import pallas as pl
from jax.experimental.pallas import tpu as pltpu
from jax.sharding import PartitionSpec as P


CLIP = 48.0
SIDES = 4
ROW, LANE = 8, 128


def coefficients(features, labels, weight):
    cls_width = weight.shape[1]
    logits = jnp.dot(features, weight, preferred_element_type=jnp.float32)
    offset = lax.axis_index("cls") * cls_width
    local_lab = labels - offset
    columns = lax.broadcasted_iota(jnp.int32, (1, cls_width), 1)
    onehot = columns == local_lab[:, None]
    label_part = jnp.sum(jnp.where(onehot, logits, 0.0), axis=1)
    top = lax.pmax(jnp.max(logits, axis=1), "cls")
    expo = jnp.exp(logits - top[:, None])
    total, squares, label_logit = lax.psum(
        (jnp.sum(expo, axis=1), jnp.sum(expo * expo, axis=1), label_part), "cls"
    )
    probs = expo / total[:, None]
    label_prob = jnp.exp(label_logit - top) / total
    resid_sq = squares / (total * total) - 2.0 * label_prob + 1.0
    resid_norm = jnp.sqrt(jnp.maximum(resid_sq, 0.0))
    feat = features.astype(jnp.float32)
    feat_norm = jnp.sqrt(jnp.sum(feat * feat, axis=1))
    factor = CLIP / jnp.maximum(feat_norm * resid_norm, CLIP)
    resid = probs - onehot.astype(jnp.float32)
    return (factor[:, None] * resid).astype(jnp.bfloat16)


def coefficient_rows(logits, rows, label):
    f32 = jnp.float32
    top = jnp.max(logits, axis=1, keepdims=True)
    expo = jnp.exp(logits - top)
    onehot = lax.broadcasted_iota(jnp.int32, logits.shape, 1) == label
    rest = jnp.where(onehot, 0.0, expo)
    total = jnp.sum(expo, axis=1, keepdims=True)
    others = jnp.sum(rest, axis=1, keepdims=True)
    squares = jnp.sum(rest * rest, axis=1, keepdims=True)
    feat = rows.astype(f32)
    feat_sq = jnp.sum(feat * feat, axis=1, keepdims=True)
    norm = jnp.sqrt(feat_sq) * jnp.sqrt(squares + others * others) / total
    gain = CLIP / jnp.maximum(norm, CLIP) / total
    return (jnp.where(onehot, -others, expo) * gain).astype(jnp.bfloat16)


def head_kernel(shape, feat_ref, label_ref, weight_ref, *refs):
    block, part, slab, skip, columns, cuts = shape
    groups = len(columns)
    outs = refs[:groups], refs[groups : 2 * groups]
    feat, wgt, coef, even, odd, sent, kept, feat_sem, wgt_sem, out_sem = refs[2 * groups :]
    blocks = feat.shape[0] // block
    logits = even, odd

    def load_rows(i):
        at = pl.ds(i * block, block)
        return pltpu.make_async_copy(feat_ref.at[at], feat.at[at], feat_sem.at[i])

    def load_columns(i):
        at = pl.ds(cuts[i], cuts[i + 1] - cuts[i])
        return pltpu.make_async_copy(weight_ref.at[:, at], wgt.at[:, at], wgt_sem.at[i])

    load_rows(0).start()
    for i in range(len(cuts) - 1):
        load_columns(i).start()
    for i in range(1, blocks):
        load_rows(i).start()
    load_rows(0).wait()
    for i in range(len(cuts) - 1):
        load_columns(i).wait()
        even[:, cuts[i] : cuts[i + 1]] = jnp.dot(
            feat[:block, :], wgt[:, cuts[i] : cuts[i + 1]], preferred_element_type=jnp.float32
        )
    for i in range(1, blocks):
        load_rows(i).wait()

    def residuals(i):
        for j in range(block // part):
            r = i * block + j * part
            line = label_ref[r // LANE : r // LANE + 1, :]
            label = jnp.broadcast_to(line, (LANE, LANE)).T[:, :1]
            coef[r : r + part, :] = coefficient_rows(
                logits[i % 2][j * part : (j + 1) * part, :], feat[r : r + part, :], label
            )

    for i in range(1, blocks):
        logits[i % 2][...] = jnp.dot(
            feat[i * block : (i + 1) * block, :], wgt[...], preferred_element_type=jnp.float32
        )
        residuals(i - 1)
    residuals(blocks - 1)

    tiles = slab // LANE
    copies = []
    for side, buf in enumerate((sent, kept)):
        core = lax.axis_index("ex") % 2
        which = core if side else 1 - core
        base = which * (feat_ref.shape[1] - slab)
        for m in range(tiles):
            off = pl.multiple_of(base + m * LANE, LANE)
            buf[m * LANE : (m + 1) * LANE, :] = lax.dot_general(
                feat[:, pl.ds(off, LANE)],
                coef[...],
                (((0,), (0,)), ((), ())),
                preferred_element_type=jnp.float32,
            ).astype(buf.dtype)
            low, high = max(0, m * LANE - skip), (m + 1) * LANE - skip
            source = pl.ds(pl.multiple_of(which * skip + low, ROW), high - low)
            for g, (first, width) in enumerate(columns):
                copies.append(
                    pltpu.make_async_copy(
                        buf.at[source, pl.ds(first, width)],
                        outs[side][g].at[pl.ds(low, high - low)],
                        out_sem.at[len(copies)],
                    )
                )
                copies[-1].start()
    for copy in copies:
        copy.wait()


def halves(features, labels, weight, columns):
    n, depth = features.shape
    width = weight.shape[1]
    half = depth // 2
    slab = -(-half // LANE) * LANE
    bf16, f32 = jnp.bfloat16, jnp.float32
    block = 2 * LANE if n % (2 * LANE) == 0 else LANE
    chunks = min(4, width // LANE)
    cuts = [round(width // LANE * i / chunks) * LANE for i in range(chunks + 1)]
    shape = block, LANE, slab, slab - half, columns, cuts
    anywhere = pl.BlockSpec(memory_space=pl.ANY)
    return pl.pallas_call(
        functools.partial(head_kernel, shape),
        in_specs=[anywhere, pl.BlockSpec(memory_space=pltpu.VMEM), anywhere],
        out_specs=[anywhere] * (2 * len(columns)),
        out_shape=[jax.ShapeDtypeStruct((half, w), bf16) for _, w in columns]
        + [jax.ShapeDtypeStruct((half, w), f32) for _, w in columns],
        scratch_shapes=[
            pltpu.VMEM((n, depth), bf16),
            pltpu.VMEM((depth, width), bf16),
            pltpu.VMEM((n, width), bf16),
            pltpu.VMEM((block, width), f32),
            pltpu.VMEM((block, width), f32),
            pltpu.VMEM((slab, width), bf16),
            pltpu.VMEM((slab, width), f32),
            pltpu.SemaphoreType.DMA((n // block,)),
            pltpu.SemaphoreType.DMA((chunks,)),
            pltpu.SemaphoreType.DMA((2 * slab // LANE * len(columns),)),
        ],
        compiler_params=pltpu.CompilerParams(vmem_limit_bytes=60 << 20),
        cost_estimate=pl.CostEstimate(
            flops=4 * n * depth * width,
            bytes_accessed=2 * n * depth + 5 * depth * width,
            transcendentals=n * width,
        ),
        name="halves",
    )(features, labels.reshape(n // LANE, LANE), weight)


def place(blocks, rows, columns, shape, into=None):
    count = len(blocks)

    def kernel(*refs):
        firsts = rows()
        out_ref = refs[-count - 3]
        held, load_sem, save_sem = refs[-count - 2 : -2], refs[-2], refs[-1]
        loads, saves = [], []
        for i in range(count):
            start = pl.multiple_of(firsts[i], ROW)
            at = out_ref.at[pl.ds(start, blocks[i].shape[0]), pl.ds(columns[i], blocks[i].shape[1])]
            loads.append(pltpu.make_async_copy(refs[i], held[i], load_sem.at[i]))
            saves.append(pltpu.make_async_copy(held[i], at, save_sem.at[i]))
        for load in loads:
            load.start()
        for load, save in zip(loads, saves):
            load.wait()
            save.start()
        for save in saves:
            save.wait()

    extra = () if into is None else (into,)
    anywhere = pl.BlockSpec(memory_space=pl.ANY)
    return pl.pallas_call(
        kernel,
        in_specs=[anywhere] * (count + len(extra)),
        out_specs=anywhere,
        out_shape=jax.ShapeDtypeStruct(shape, blocks[0].dtype),
        scratch_shapes=[pltpu.VMEM(b.shape, b.dtype) for b in blocks]
        + [pltpu.SemaphoreType.DMA((count,)), pltpu.SemaphoreType.DMA((count,))],
        input_output_aliases={count: 0} if extra else {},
        compiler_params=pltpu.CompilerParams(vmem_limit_bytes=16 << 20),
        name="place",
    )(*blocks, *extra)


class Cut:
    def __init__(self, total, pieces):
        self.own, self.pieces = total // pieces, pieces
        firsts = [self.own * k // ROW * ROW for k in range(pieces)]
        lasts = [-(-self.own * (k + 1) // ROW) * ROW for k in range(pieces)]
        self.count = max(last - first for first, last in zip(firsts, lasts))
        self.most = total - self.count
        self.skips = [self.own * k - min(f, self.most) for k, f in enumerate(firsts)]

    def start(self, k):
        first = self.own * k
        return lax.min(first - lax.rem(first, ROW), jnp.int32(self.most))


def rows_of(x, start, count):
    return lax.dynamic_slice_in_dim(x, start, count, 0)


def narrow_share(width):
    tiles = width // LANE
    return max(1, round(tiles * 3 / 11)) * LANE


class Group:
    def __init__(self, stride, count):
        n = lax.axis_size("ex")
        self.count = count
        self.index = lax.axis_index("ex") // stride % count
        self.pairs = [[(i, i ^ (stride * d)) for i in range(n)] for d in range(count)]

    def swap(self, x, d):
        return lax.ppermute(x, "ex", self.pairs[d])

    def sum(self, rows_at):
        got = []
        for d in reversed(range(1, self.count)):
            sent = rows_at(self.index ^ d).astype(jnp.bfloat16)
            got.append(self.swap(sent, d))
        total = rows_at(self.index)
        for part in got:
            total = total + part.astype(jnp.float32)
        return total

    def spread(self, x):
        return [x] + [self.swap(x, d) for d in range(1, self.count)]


def two_way(core):
    return [jnp.where(core == 0, 2, 1), jnp.where(core == 0, 1, 2), 3]


def two_way_swaps():
    n = lax.axis_size("ex")
    first = [(i, i ^ (4 if i % 2 else 2)) for i in range(n)]
    second = [(i, i ^ (2 if i % 2 else 4)) for i in range(n)]
    return first, second


def two_way_sum(core, side, rows_at):
    bf16, f32 = jnp.bfloat16, jnp.float32
    first, second = two_way_swaps()
    second_d, first_d, far_d = two_way(core)

    def at(d):
        return rows_at(side.index ^ d)

    sent = jnp.concatenate([at(far_d).astype(bf16), at(first_d).astype(bf16)], axis=0)
    got = lax.ppermute(sent, "ex", first)
    count = sent.shape[0] // 2
    passed = (at(second_d) + got[:count].astype(f32)).astype(bf16)
    last = lax.ppermute(passed, "ex", second)
    return at(0) + got[count:].astype(f32) + last.astype(f32)


def two_way_spread(x):
    first, second = two_way_swaps()
    from_second = lax.ppermute(x, "ex", second)
    from_first = lax.ppermute(x, "ex", first)
    far = lax.ppermute(from_second, "ex", first)
    return [from_second, from_first, far]


def join(parts, index, cut):
    ordered = []
    for k, skip in enumerate(cut.skips):
        which = jnp.broadcast_to(index ^ k, parts[0].shape)
        piece = lax.select_n(which.astype(jnp.int32), *parts)
        ordered.append(piece[skip : skip + cut.own])
    return jnp.concatenate(ordered, axis=0)


def by_rows(features, labels, weight, noise):
    bf16, f32 = jnp.bfloat16, jnp.float32
    n = lax.axis_size("ex")
    layers = n // (2 * SIDES)
    core, side, layer = Group(1, 2), Group(2, SIDES), Group(2 * SIDES, layers)
    depth, width = weight.shape
    half, own = depth // 2, depth // n
    by_side, by_layer = half // SIDES, half // layers
    narrow = narrow_share(width)
    wide = width - narrow
    classes = width * lax.axis_size("cls")
    batch = features.shape[0] * n
    scale = 0.1 * classes / batch

    to_wide, to_narrow = [], []
    for d in range(n):
        c, rest = d // (SIDES * layers), d % (SIDES * layers)
        q, k = rest // layers, rest % layers
        to_wide.append((d, (k * SIDES + q) * 2 + c))
        k, q = rest // SIDES, rest % SIDES
        to_narrow.append((d, (k * SIDES + q) * 2 + c))

    wide_cut, narrow_cut = Cut(by_side, layers), Cut(by_layer, SIDES)

    def shifted(noise_own, cut, index):
        shapes = []
        for skip in cut.skips:
            shapes.append(jnp.pad(noise_own, ((skip, cut.count - own - skip), (0, 0))))
        which = jnp.broadcast_to(index, shapes[0].shape)
        return lax.select_n(which.astype(jnp.int32), *shapes)

    def updated(grad, noise_rows, begin, columns):
        rows = lax.dynamic_slice(weight, (begin, jnp.int32(columns)), grad.shape)
        return (
            rows.astype(f32) - scale * (grad + 0.96 * CLIP * noise_rows.astype(f32))
        ).astype(bf16)

    columns = [(wide, narrow), (0, wide)]
    if lax.axis_size("cls") == 1 and features.shape[0] % LANE == 0:
        sent_n, sent_w, kept_n, kept_w = halves(
            features, labels, weight, columns
        )
    else:
        coef = coefficients(features, labels, weight)
        grad = lax.dot_general(
            features, coef, (((0,), (0,)), ((), ())), preferred_element_type=f32
        )
        sent = rows_of(grad, half * (1 - core.index), half).astype(bf16)
        kept = rows_of(grad, half * core.index, half)
        sent_n, sent_w = sent[:, wide:], sent[:, :wide]
        kept_n, kept_w = kept[:, wide:], kept[:, :wide]

    got_n = core.swap(sent_n, 1)
    got_w = core.swap(sent_w, 1)
    noise, kept_n, kept_w = lax.optimization_barrier((noise, kept_n, kept_w))
    noise_n = lax.ppermute(noise[:, wide:], "ex", to_narrow)
    noise_w = lax.ppermute(noise[:, :wide], "ex", to_wide)

    def narrow_rows(k):
        start = by_layer * k
        return rows_of(kept_n, start, by_layer) + rows_of(got_n, start, by_layer).astype(f32)

    def wide_rows(k):
        start = by_side * k
        return rows_of(kept_w, start, by_side) + rows_of(got_w, start, by_side).astype(f32)

    layer_sum = layer.sum(narrow_rows)
    side_sum = two_way_sum(core.index, side, wide_rows)
    layer_sum, side_sum = lax.optimization_barrier((layer_sum, side_sum))
    noise_n = shifted(noise_n, narrow_cut, side.index)
    noise_w = shifted(noise_w, wide_cut, layer.index)
    noise_n, noise_w = lax.optimization_barrier((noise_n, noise_w))
    grad_n = side.sum(lambda k: rows_of(layer_sum, narrow_cut.start(k), narrow_cut.count))
    grad_w = layer.sum(lambda k: rows_of(side_sum, wide_cut.start(k), wide_cut.count))

    begin = half * core.index + by_layer * layer.index + narrow_cut.start(side.index)
    new_narrow = updated(grad_n, noise_n, begin, wide)
    begin = half * core.index + by_side * side.index + wide_cut.start(layer.index)
    new_wide = updated(grad_w, noise_w, begin, 0)
    new_narrow, new_wide = lax.optimization_barrier((new_narrow, new_wide))
    layer_parts, side_parts = lax.optimization_barrier(
        (side.spread(new_narrow), layer.spread(new_wide))
    )
    layer_block = join(layer_parts, side.index, narrow_cut)
    side_block = join(side_parts, layer.index, wide_cut)
    near = [layer_block, side_block]
    near += [core.swap(b, 1) for b in near]

    def rows_in(of_core):
        def rows():
            at = lax.axis_index("ex")
            c = at % 2 if of_core == 0 else 1 - at % 2
            q, k = at // 2 % SIDES, at // (2 * SIDES)
            narrow_at = [half * c + by_layer * (k ^ d) for d in range(layers)]
            wide_at = [half * c + by_side * (q ^ d) for d in [0] + two_way(c)]
            return narrow_at, wide_at

        return rows

    def near_rows():
        (a, b), (c, d) = rows_in(0)(), rows_in(1)()
        return [a[0], b[0], c[0], d[0]]

    def early_rows():
        (_, b), (_, d) = rows_in(0)(), rows_in(1)()
        return b[1:3] + d[1:3]

    def narrow_rows_late():
        (a, _), (c, _) = rows_in(0)(), rows_in(1)()
        return a[1:] + c[1:]

    def last_rows():
        (_, b), (_, d) = rows_in(0)(), rows_in(1)()
        return [b[3], d[3]]

    out = place(near, near_rows, [wide, 0] * 2, weight.shape)

    blocks = layer.spread(layer_block)[1:]
    side_blocks = two_way_spread(side_block)
    last_far = core.swap(side_blocks[2], 1)
    side_blocks += [core.swap(b, 1) for b in side_blocks[:2]] + [last_far]
    early = [side_blocks[i] for i in (0, 1, 3, 4)]
    out = place(early, early_rows, [0] * 4, weight.shape, out)
    blocks += [core.swap(b, 1) for b in blocks]
    out = place(blocks, narrow_rows_late, [wide] * len(blocks), weight.shape, out)
    last = [side_blocks[2], side_blocks[5]]
    return place(last, last_rows, [0] * 2, weight.shape, out)


def by_columns(features, labels, weight, noise):
    coef = coefficients(features, labels, weight)
    partial_grad = lax.dot_general(
        features, coef, (((0,), (0,)), ((), ())), preferred_element_type=jnp.float32
    )
    classes = weight.shape[1] * lax.axis_size("cls")
    batch = features.shape[0] * lax.axis_size("ex")
    scale = 0.1 * classes / batch
    grad_part = lax.psum_scatter(partial_grad, "ex", scatter_dimension=0, tiled=True)
    span = grad_part.shape[0]
    own_weight = lax.dynamic_slice_in_dim(weight, lax.axis_index("ex") * span, span, 0)
    updated = own_weight.astype(jnp.float32) - scale * (
        grad_part + 0.96 * CLIP * noise.astype(jnp.float32)
    )
    return lax.all_gather(updated.astype(jnp.bfloat16), "ex", axis=0, tiled=True)


def local(features, labels, weight, noise):
    n = lax.axis_size("ex")
    depth, width = weight.shape
    layers = n // (2 * SIDES)
    fits = n % (2 * SIDES) == 0 and layers > 1 and layers & (layers - 1) == 0
    fits = fits and depth % n == 0 and width % LANE == 0 and width > LANE
    fits = fits and depth % (2 * ROW * SIDES) == 0 and depth % (2 * ROW * layers) == 0
    if not fits:
        return by_columns(features, labels, weight, noise)
    return by_rows(features, labels, weight, noise)


def solution(mesh):
    in_specs = (P("ex", None), P("ex"), P(None, "cls"), P("ex", "cls"))
    out_specs = P(None, "cls")
    return jax.shard_map(
        local, mesh=mesh, in_specs=in_specs, out_specs=out_specs, check_vma=False
    )
```

```python
import functools

import jax
import jax.numpy as jnp
from jax import lax
from jax.experimental import pallas as pl
from jax.experimental.pallas import tpu as pltpu
from jax.sharding import PartitionSpec as P


CLIP = 48.0
SIDES = 4
ROW, LANE = 8, 128


def coefficients(features, labels, weight):
    cls_width = weight.shape[1]
    logits = jnp.dot(features, weight, preferred_element_type=jnp.float32)
    offset = lax.axis_index("cls") * cls_width
    local_lab = labels - offset
    columns = lax.broadcasted_iota(jnp.int32, (1, cls_width), 1)
    onehot = columns == local_lab[:, None]
    label_part = jnp.sum(jnp.where(onehot, logits, 0.0), axis=1)
    top = lax.pmax(jnp.max(logits, axis=1), "cls")
    expo = jnp.exp(logits - top[:, None])
    total, squares, label_logit = lax.psum(
        (jnp.sum(expo, axis=1), jnp.sum(expo * expo, axis=1), label_part), "cls"
    )
    probs = expo / total[:, None]
    label_prob = jnp.exp(label_logit - top) / total
    resid_sq = squares / (total * total) - 2.0 * label_prob + 1.0
    resid_norm = jnp.sqrt(jnp.maximum(resid_sq, 0.0))
    feat = features.astype(jnp.float32)
    feat_norm = jnp.sqrt(jnp.sum(feat * feat, axis=1))
    factor = CLIP / jnp.maximum(feat_norm * resid_norm, CLIP)
    resid = probs - onehot.astype(jnp.float32)
    return (factor[:, None] * resid).astype(jnp.bfloat16)


def coefficient_rows(logits, rows, label):
    f32 = jnp.float32
    top = jnp.max(logits, axis=1, keepdims=True)
    expo = jnp.exp(logits - top)
    onehot = lax.broadcasted_iota(jnp.int32, logits.shape, 1) == label
    rest = jnp.where(onehot, 0.0, expo)
    total = jnp.sum(expo, axis=1, keepdims=True)
    others = jnp.sum(rest, axis=1, keepdims=True)
    squares = jnp.sum(rest * rest, axis=1, keepdims=True)
    feat = rows.astype(f32)
    feat_sq = jnp.sum(feat * feat, axis=1, keepdims=True)
    norm = jnp.sqrt(feat_sq) * jnp.sqrt(squares + others * others) / total
    gain = CLIP / jnp.maximum(norm, CLIP) / total
    return (jnp.where(onehot, -others, expo) * gain).astype(jnp.bfloat16)


def head_kernel(shape, feat_ref, label_ref, weight_ref, *refs):
    block, part, slab, skip, columns, cuts = shape
    groups = len(columns)
    outs = refs[:groups], refs[groups : 2 * groups]
    feat, wgt, coef, even, odd, sent, kept, feat_sem, wgt_sem, out_sem = refs[2 * groups :]
    blocks = feat.shape[0] // block
    logits = even, odd

    def load_rows(i):
        at = pl.ds(i * block, block)
        return pltpu.make_async_copy(feat_ref.at[at], feat.at[at], feat_sem.at[i])

    def load_columns(i):
        at = pl.ds(cuts[i], cuts[i + 1] - cuts[i])
        return pltpu.make_async_copy(weight_ref.at[:, at], wgt.at[:, at], wgt_sem.at[i])

    load_rows(0).start()
    for i in range(len(cuts) - 1):
        load_columns(i).start()
    for i in range(1, blocks):
        load_rows(i).start()
    load_rows(0).wait()
    for i in range(len(cuts) - 1):
        load_columns(i).wait()
        even[:, cuts[i] : cuts[i + 1]] = jnp.dot(
            feat[:block, :], wgt[:, cuts[i] : cuts[i + 1]], preferred_element_type=jnp.float32
        )
    for i in range(1, blocks):
        load_rows(i).wait()

    def residuals(i):
        for j in range(block // part):
            r = i * block + j * part
            line = label_ref[r // LANE : r // LANE + 1, :]
            label = jnp.broadcast_to(line, (LANE, LANE)).T[:, :1]
            coef[r : r + part, :] = coefficient_rows(
                logits[i % 2][j * part : (j + 1) * part, :], feat[r : r + part, :], label
            )

    for i in range(1, blocks):
        logits[i % 2][...] = jnp.dot(
            feat[i * block : (i + 1) * block, :], wgt[...], preferred_element_type=jnp.float32
        )
        residuals(i - 1)
    residuals(blocks - 1)

    tiles = slab // LANE
    copies = []
    for side, buf in enumerate((sent, kept)):
        core = lax.axis_index("ex") % 2
        which = core if side else 1 - core
        base = which * (feat_ref.shape[1] - slab)
        for m in range(tiles):
            off = pl.multiple_of(base + m * LANE, LANE)
            buf[m * LANE : (m + 1) * LANE, :] = lax.dot_general(
                feat[:, pl.ds(off, LANE)],
                coef[...],
                (((0,), (0,)), ((), ())),
                preferred_element_type=jnp.float32,
            ).astype(buf.dtype)
            low, high = max(0, m * LANE - skip), (m + 1) * LANE - skip
            source = pl.ds(pl.multiple_of(which * skip + low, ROW), high - low)
            for g, (first, width) in enumerate(columns):
                copies.append(
                    pltpu.make_async_copy(
                        buf.at[source, pl.ds(first, width)],
                        outs[side][g].at[pl.ds(low, high - low)],
                        out_sem.at[len(copies)],
                    )
                )
                copies[-1].start()
    for copy in copies:
        copy.wait()


def halves(features, labels, weight, columns):
    n, depth = features.shape
    width = weight.shape[1]
    half = depth // 2
    slab = -(-half // LANE) * LANE
    bf16, f32 = jnp.bfloat16, jnp.float32
    block = 2 * LANE if n % (2 * LANE) == 0 else LANE
    chunks = min(4, width // LANE)
    cuts = [round(width // LANE * i / chunks) * LANE for i in range(chunks + 1)]
    shape = block, LANE, slab, slab - half, columns, cuts
    anywhere = pl.BlockSpec(memory_space=pl.ANY)
    return pl.pallas_call(
        functools.partial(head_kernel, shape),
        in_specs=[anywhere, pl.BlockSpec(memory_space=pltpu.VMEM), anywhere],
        out_specs=[anywhere] * (2 * len(columns)),
        out_shape=[jax.ShapeDtypeStruct((half, w), bf16) for _, w in columns]
        + [jax.ShapeDtypeStruct((half, w), f32) for _, w in columns],
        scratch_shapes=[
            pltpu.VMEM((n, depth), bf16),
            pltpu.VMEM((depth, width), bf16),
            pltpu.VMEM((n, width), bf16),
            pltpu.VMEM((block, width), f32),
            pltpu.VMEM((block, width), f32),
            pltpu.VMEM((slab, width), bf16),
            pltpu.VMEM((slab, width), f32),
            pltpu.SemaphoreType.DMA((n // block,)),
            pltpu.SemaphoreType.DMA((chunks,)),
            pltpu.SemaphoreType.DMA((2 * slab // LANE * len(columns),)),
        ],
        compiler_params=pltpu.CompilerParams(vmem_limit_bytes=60 << 20),
        cost_estimate=pl.CostEstimate(
            flops=4 * n * depth * width,
            bytes_accessed=2 * n * depth + 5 * depth * width,
            transcendentals=n * width,
        ),
        name="halves",
    )(features, labels.reshape(n // LANE, LANE), weight)


def place(blocks, rows, columns, shape, into=None):
    count = len(blocks)

    def kernel(*refs):
        firsts = rows()
        out_ref = refs[-count - 3]
        held, load_sem, save_sem = refs[-count - 2 : -2], refs[-2], refs[-1]
        loads, saves = [], []
        for i in range(count):
            start = pl.multiple_of(firsts[i], ROW)
            at = out_ref.at[pl.ds(start, blocks[i].shape[0]), pl.ds(columns[i], blocks[i].shape[1])]
            loads.append(pltpu.make_async_copy(refs[i], held[i], load_sem.at[i]))
            saves.append(pltpu.make_async_copy(held[i], at, save_sem.at[i]))
        for load in loads:
            load.start()
        for load, save in zip(loads, saves):
            load.wait()
            save.start()
        for save in saves:
            save.wait()

    extra = () if into is None else (into,)
    anywhere = pl.BlockSpec(memory_space=pl.ANY)
    return pl.pallas_call(
        kernel,
        in_specs=[anywhere] * (count + len(extra)),
        out_specs=anywhere,
        out_shape=jax.ShapeDtypeStruct(shape, blocks[0].dtype),
        scratch_shapes=[pltpu.VMEM(b.shape, b.dtype) for b in blocks]
        + [pltpu.SemaphoreType.DMA((count,)), pltpu.SemaphoreType.DMA((count,))],
        input_output_aliases={count: 0} if extra else {},
        compiler_params=pltpu.CompilerParams(vmem_limit_bytes=16 << 20),
        name="place",
    )(*blocks, *extra)


class Cut:
    def __init__(self, total, pieces):
        self.own, self.pieces = total // pieces, pieces
        firsts = [self.own * k // ROW * ROW for k in range(pieces)]
        lasts = [-(-self.own * (k + 1) // ROW) * ROW for k in range(pieces)]
        self.count = max(last - first for first, last in zip(firsts, lasts))
        self.most = total - self.count
        self.skips = [self.own * k - min(f, self.most) for k, f in enumerate(firsts)]

    def start(self, k):
        first = self.own * k
        return lax.min(first - lax.rem(first, ROW), jnp.int32(self.most))


def rows_of(x, start, count):
    return lax.dynamic_slice_in_dim(x, start, count, 0)


def narrow_share(width):
    tiles = width // LANE
    return max(1, round(tiles * 3 / 11)) * LANE


class Group:
    def __init__(self, stride, count):
        n = lax.axis_size("ex")
        self.count = count
        self.index = lax.axis_index("ex") // stride % count
        self.pairs = [[(i, i ^ (stride * d)) for i in range(n)] for d in range(count)]

    def swap(self, x, d):
        return lax.ppermute(x, "ex", self.pairs[d])

    def sum(self, rows_at):
        got = []
        for d in reversed(range(1, self.count)):
            sent = rows_at(self.index ^ d).astype(jnp.bfloat16)
            got.append(self.swap(sent, d))
        total = rows_at(self.index)
        for part in got:
            total = total + part.astype(jnp.float32)
        return total

    def spread(self, x):
        return [x] + [self.swap(x, d) for d in range(1, self.count)]


def two_way(core):
    return [jnp.where(core == 0, 2, 1), jnp.where(core == 0, 1, 2), 3]


def two_way_swaps():
    n = lax.axis_size("ex")
    first = [(i, i ^ (4 if i % 2 else 2)) for i in range(n)]
    second = [(i, i ^ (2 if i % 2 else 4)) for i in range(n)]
    return first, second


def two_way_sum(core, side, rows_at):
    bf16, f32 = jnp.bfloat16, jnp.float32
    first, second = two_way_swaps()
    second_d, first_d, far_d = two_way(core)

    def at(d):
        return rows_at(side.index ^ d)

    far, near = at(far_d).astype(bf16), at(first_d).astype(bf16)
    got_far = lax.ppermute(far, "ex", first)
    got_near = lax.ppermute(near, "ex", first)
    passed = (at(second_d) + got_far.astype(f32)).astype(bf16)
    last = lax.ppermute(passed, "ex", second)
    return at(0) + got_near.astype(f32) + last.astype(f32)


def two_way_spread(x):
    first, second = two_way_swaps()
    from_second = lax.ppermute(x, "ex", second)
    from_first = lax.ppermute(x, "ex", first)
    far = lax.ppermute(from_second, "ex", first)
    return [from_second, from_first, far]


def join(parts, index, cut):
    ordered = []
    for k, skip in enumerate(cut.skips):
        which = jnp.broadcast_to(index ^ k, parts[0].shape)
        piece = lax.select_n(which.astype(jnp.int32), *parts)
        ordered.append(piece[skip : skip + cut.own])
    return jnp.concatenate(ordered, axis=0)


def by_rows(features, labels, weight, noise):
    bf16, f32 = jnp.bfloat16, jnp.float32
    n = lax.axis_size("ex")
    layers = n // (2 * SIDES)
    core, side, layer = Group(1, 2), Group(2, SIDES), Group(2 * SIDES, layers)
    depth, width = weight.shape
    half, own = depth // 2, depth // n
    by_side, by_layer = half // SIDES, half // layers
    narrow = narrow_share(width)
    wide = width - narrow
    classes = width * lax.axis_size("cls")
    batch = features.shape[0] * n
    scale = 0.1 * classes / batch

    to_wide, to_narrow = [], []
    for d in range(n):
        c, rest = d // (SIDES * layers), d % (SIDES * layers)
        q, k = rest // layers, rest % layers
        to_wide.append((d, (k * SIDES + q) * 2 + c))
        k, q = rest // SIDES, rest % SIDES
        to_narrow.append((d, (k * SIDES + q) * 2 + c))

    wide_cut, narrow_cut = Cut(by_side, layers), Cut(by_layer, SIDES)

    def shifted(noise_own, cut, index):
        shapes = []
        for skip in cut.skips:
            shapes.append(jnp.pad(noise_own, ((skip, cut.count - own - skip), (0, 0))))
        which = jnp.broadcast_to(index, shapes[0].shape)
        return lax.select_n(which.astype(jnp.int32), *shapes)

    def updated(grad, noise_rows, begin, columns):
        rows = lax.dynamic_slice(weight, (begin, jnp.int32(columns)), grad.shape)
        return (
            rows.astype(f32) - scale * (grad + 0.96 * CLIP * noise_rows.astype(f32))
        ).astype(bf16)

    columns = [(wide, narrow), (0, wide)]
    if lax.axis_size("cls") == 1 and features.shape[0] % LANE == 0:
        sent_n, sent_w, kept_n, kept_w = halves(
            features, labels, weight, columns
        )
    else:
        coef = coefficients(features, labels, weight)
        grad = lax.dot_general(
            features, coef, (((0,), (0,)), ((), ())), preferred_element_type=f32
        )
        sent = rows_of(grad, half * (1 - core.index), half).astype(bf16)
        kept = rows_of(grad, half * core.index, half)
        sent_n, sent_w = sent[:, wide:], sent[:, :wide]
        kept_n, kept_w = kept[:, wide:], kept[:, :wide]

    got_n = core.swap(sent_n, 1)
    got_w = core.swap(sent_w, 1)
    noise, kept_n, kept_w = lax.optimization_barrier((noise, kept_n, kept_w))
    noise_n = lax.ppermute(noise[:, wide:], "ex", to_narrow)
    noise_w = lax.ppermute(noise[:, :wide], "ex", to_wide)

    def narrow_rows(k):
        start = by_layer * k
        return rows_of(kept_n, start, by_layer) + rows_of(got_n, start, by_layer).astype(f32)

    def wide_rows(k):
        start = by_side * k
        return rows_of(kept_w, start, by_side) + rows_of(got_w, start, by_side).astype(f32)

    layer_sum = layer.sum(narrow_rows)
    side_sum = two_way_sum(core.index, side, wide_rows)
    layer_sum, side_sum = lax.optimization_barrier((layer_sum, side_sum))
    noise_n = shifted(noise_n, narrow_cut, side.index)
    noise_w = shifted(noise_w, wide_cut, layer.index)
    noise_n, noise_w = lax.optimization_barrier((noise_n, noise_w))
    grad_n = side.sum(lambda k: rows_of(layer_sum, narrow_cut.start(k), narrow_cut.count))
    grad_w = layer.sum(lambda k: rows_of(side_sum, wide_cut.start(k), wide_cut.count))

    begin = half * core.index + by_layer * layer.index + narrow_cut.start(side.index)
    new_narrow = updated(grad_n, noise_n, begin, wide)
    begin = half * core.index + by_side * side.index + wide_cut.start(layer.index)
    new_wide = updated(grad_w, noise_w, begin, 0)
    new_narrow, new_wide = lax.optimization_barrier((new_narrow, new_wide))
    layer_parts, side_parts = lax.optimization_barrier(
        (side.spread(new_narrow), layer.spread(new_wide))
    )
    layer_block = join(layer_parts, side.index, narrow_cut)
    side_block = join(side_parts, layer.index, wide_cut)
    near = [layer_block, side_block]
    near += [core.swap(b, 1) for b in near]

    def rows_in(of_core):
        def rows():
            at = lax.axis_index("ex")
            c = at % 2 if of_core == 0 else 1 - at % 2
            q, k = at // 2 % SIDES, at // (2 * SIDES)
            narrow_at = [half * c + by_layer * (k ^ d) for d in range(layers)]
            wide_at = [half * c + by_side * (q ^ d) for d in [0] + two_way(c)]
            return narrow_at, wide_at

        return rows

    def near_rows():
        (a, b), (c, d) = rows_in(0)(), rows_in(1)()
        return [a[0], b[0], c[0], d[0]]

    def early_rows():
        (_, b), (_, d) = rows_in(0)(), rows_in(1)()
        return b[1:3] + d[1:3]

    def narrow_rows_late():
        (a, _), (c, _) = rows_in(0)(), rows_in(1)()
        return a[1:] + c[1:]

    def last_rows():
        (_, b), (_, d) = rows_in(0)(), rows_in(1)()
        return [b[3], d[3]]

    out = place(near, near_rows, [wide, 0] * 2, weight.shape)

    blocks = layer.spread(layer_block)[1:]
    side_blocks = two_way_spread(side_block)
    last_far = core.swap(side_blocks[2], 1)
    side_blocks += [core.swap(b, 1) for b in side_blocks[:2]] + [last_far]
    early = [side_blocks[i] for i in (0, 1, 3, 4)]
    out = place(early, early_rows, [0] * 4, weight.shape, out)
    blocks += [core.swap(b, 1) for b in blocks]
    out = place(blocks, narrow_rows_late, [wide] * len(blocks), weight.shape, out)
    last = [side_blocks[2], side_blocks[5]]
    return place(last, last_rows, [0] * 2, weight.shape, out)


def by_columns(features, labels, weight, noise):
    coef = coefficients(features, labels, weight)
    partial_grad = lax.dot_general(
        features, coef, (((0,), (0,)), ((), ())), preferred_element_type=jnp.float32
    )
    classes = weight.shape[1] * lax.axis_size("cls")
    batch = features.shape[0] * lax.axis_size("ex")
    scale = 0.1 * classes / batch
    grad_part = lax.psum_scatter(partial_grad, "ex", scatter_dimension=0, tiled=True)
    span = grad_part.shape[0]
    own_weight = lax.dynamic_slice_in_dim(weight, lax.axis_index("ex") * span, span, 0)
    updated = own_weight.astype(jnp.float32) - scale * (
        grad_part + 0.96 * CLIP * noise.astype(jnp.float32)
    )
    return lax.all_gather(updated.astype(jnp.bfloat16), "ex", axis=0, tiled=True)


def local(features, labels, weight, noise):
    n = lax.axis_size("ex")
    depth, width = weight.shape
    layers = n // (2 * SIDES)
    fits = n % (2 * SIDES) == 0 and layers > 1 and layers & (layers - 1) == 0
    fits = fits and depth % n == 0 and width % LANE == 0 and width > LANE
    fits = fits and depth % (2 * ROW * SIDES) == 0 and depth % (2 * ROW * layers) == 0
    if not fits:
        return by_columns(features, labels, weight, noise)
    return by_rows(features, labels, weight, noise)


def solution(mesh):
    in_specs = (P("ex", None), P("ex"), P(None, "cls"), P("ex", "cls"))
    out_specs = P(None, "cls")
    return jax.shard_map(
        local, mesh=mesh, in_specs=in_specs, out_specs=out_specs, check_vma=False
    )
```
